128 devices in a mesh: gx: 32 (over y, x, core), gy: 4 (over z).
Axes of the slice: x: 4, y: 4, z: 4, core: 2. Of those that a mesh axis runs over, the one named last changes fastest.
Arguments:
- sources: bfloat16 [8192, 8, 128], P(('gx', 'gy')), may hold values from -6 to 6
- owners: int32 [8192, 1], P(('gx', 'gy')), may hold values from 0 to 31; in each aligned block of 64 rows (0 to 63, 64 to 127, ...) at most 4 rows name the same one
- strip_rows: int32 [8192], P(('gx', 'gy')), may hold values from 0 to 255
- panel_counts: int32 [8192], P(('gx', 'gy')), may hold values from 1 to 128
- arrival_bins: int32 [8192, 4, 128], P('gx'), may hold values from 0 to 254
- arrival_fracs: float32 [8192, 4, 128], P('gx'), may hold values from 0 to 1
- gain_table: bfloat16 [8192, 8, 4, 1024], P('gx'), may hold values from -0.125 to 0.125
Outputs:
- signals: float32 [1024, 4, 256], P(('gx', 'gy'))
The draws below stay inside these ranges and needn't reach their ends.
Inputs may be any that keep to these rules, and one draw needn't show every extreme that they name: `owners`: among the rows of one device, at most 4 strips name one patch, a bound that some block reaches.
All inputs are finite; a program needn't handle non-finite values.
Results may differ from the reference program's by a relative error of at most 0.0044.
Values may be sent and summed in bfloat16 or wider, within the bound.
A program may use at most 768 MiB of HBM per device.

```python
import math
import jax
import jax.numpy as jnp
import numpy as np
from jax import lax

TERMS = 8
SP = 128
NBIN = 256
NOB = 4
OBS_BLOCK = 1024
STRIP_DEV = 64
ROWS = 256
CAP = 4
STRIPS = 8192
TROWS = 8192
N_GX = 32


def set_ends(array, stream_key, low, high):
    longest = array.shape.index(max(array.shape))
    spots = []
    for shift in (0, 1):
        where = [jax.random.randint(jax.random.fold_in(stream_key, axis), (), 0, length) for axis, length in enumerate(array.shape)]
        where[longest] = (where[longest] + shift) % array.shape[longest]
        spots.append(tuple(where))
    return array.at[spots[0]].set(low).at[spots[1]].set(high)


def spiked(drawn, key, source, target, shards_of, factor):
    owner, partner = [(jnp.arange(drawn.shape[axis_at]) // (drawn.shape[axis_at] // shards_of)).reshape([-1 if axis == axis_at else 1 for axis in range(drawn.ndim)]) for axis_at in (source, target)]
    chosen = jax.random.permutation(key, shards_of)[partner]
    strong = (owner == chosen) | (owner == (partner + shards_of // 2) % shards_of)
    return jnp.where(strong, factor * drawn, drawn)


def level_of(own_key, shape, pieces, low, largest):
    def one(position, parts):
        heights = jax.random.uniform(jax.random.fold_in(jax.random.fold_in(own_key, 6), position), (parts,), jnp.float32, low / len(pieces), largest / len(pieces))
        return jnp.repeat(jnp.exp(heights), shape[position] // parts).reshape((-1,) + (1,) * (len(shape) - position - 1))

    level = one(*pieces[0])
    for cut in pieces[1:]:
        level = level * one(*cut)
    return level


def assign_block(key, own, number, rows, count, top, most, slope):
    order = jax.random.permutation(key, count)
    crowded, usual = portions_of(count, rows * top, most, slope, True), portions_of(count, rows * top, most, slope, False)
    places = jnp.arange(count)

    def named(sizes, turn):
        used = int((sizes > 0).sum())
        fixed = max(1, used // 4)
        passed = fixed + (places - fixed + turn * (used - fixed)) % max(1, count - fixed)
        return jnp.zeros((count,), jnp.int32).at[order[jnp.where(places < fixed, places, passed)]].set(jnp.asarray(sizes, jnp.int32))

    sizes = jnp.where(number % 4 == 0, named(crowded, number // 4), named(usual, number - number // 4 - 1))
    mixed = jax.random.permutation(jax.random.fold_in(own, 3), count)
    donor, receiver = mixed[0:count // 2 * 2:2], mixed[1:count // 2 * 2:2]
    slack = jnp.minimum(sizes[donor] - 1, most - sizes[receiver]) // 2
    slack = jnp.where((donor == order[0]) | (receiver == order[0]) | (sizes[receiver] == 0), 0, jnp.maximum(slack, 0))
    passed = jax.random.randint(jax.random.fold_in(own, 4), (count // 2,), 0, 1 << 20) % (slack + 1)
    sizes = sizes.at[donor].add(-passed).at[receiver].add(passed)
    members = jnp.searchsorted(jnp.cumsum(sizes), jnp.arange(rows * top), side="right").astype(jnp.int32)
    listing = members.reshape(top, rows).T
    listing = listing[jax.random.permutation(jax.random.fold_in(own, 1), rows)]
    turn = jax.random.randint(jax.random.fold_in(own, 2), (rows, 1), 0, top)
    return jnp.take_along_axis(listing, (jnp.arange(top)[None, :] + turn) % top, axis=1)


def portions_of(count, total, reach, slope, full):
    loads = [(1 << 20) // math.isqrt(standing ** slope) + 1 for standing in range(1, count + 1)]
    largest = reach if full else min(reach, max(-(-total // count), total * loads[0] // sum(loads)))
    least = 1 if total - largest >= count - 1 else 0
    holding, surplus = [largest] + [least] * (count - 1), total - largest - least * (count - 1)
    while surplus > 0:
        free = [i for i in range(1, count) if holding[i] < largest] or [i for i in range(1, count) if holding[i] < reach]
        pool, budget = sum([loads[i] for i in free]), surplus
        for i in free:
            more = min(reach - holding[i], max(1, budget * loads[i] // pool), surplus)
            holding[i] = holding[i] + more
            surplus = surplus - more
    return np.array(holding)


def gaussian(rng, dims, spread, most, shards=(), held_as=jnp.bfloat16):
    values = spread * jax.random.normal(rng, dims, jnp.float32)
    if shards:
        values = values * level_of(rng, dims, shards, -0.22, 0.18)
    return jnp.clip(values, -most, most).astype(held_as)


def bell_draw_with(key, shape, width, limit, split, heavy, kind=jnp.bfloat16):
    result = width * jax.random.normal(key, shape, jnp.float32)
    if split:
        result = result * level_of(key, shape, split, -0.22, 0.18)
    return jnp.clip(spiked(result, jax.random.fold_in(key, 3), *heavy), -limit, limit).astype(kind)


def setup_inputs(seed: int = 0) -> dict:
    arg_keys = jax.random.split(jax.random.key(seed), 8)
    sources = gaussian(arg_keys[0], (STRIPS, TERMS, SP), 1.0, 6.0, ((0, 128),))
    owners_keys = jax.random.split(jax.random.fold_in(arg_keys[1], 1), STRIPS // STRIP_DEV)
    owners_turns = jax.random.permutation(jax.random.fold_in(arg_keys[1], 3), STRIPS // STRIP_DEV)
    owners = jax.vmap(lambda own, number: assign_block(jax.random.fold_in(arg_keys[1], 2), own, number, STRIP_DEV, N_GX, 1, CAP, 2))(owners_keys, owners_turns).reshape((STRIPS, 1))
    strip_rows = set_ends(jax.random.randint(arg_keys[2], (STRIPS,), 0, ROWS), jax.random.fold_in(arg_keys[2], 1), 0, ROWS - 1).astype(jnp.int32)
    panel_counts = set_ends(jax.random.randint(arg_keys[3], (STRIPS,), 1, SP + 1), jax.random.fold_in(arg_keys[3], 1), 1, SP).astype(jnp.int32)
    arrival_bins = set_ends(jax.random.randint(arg_keys[4], (TROWS, NOB, SP), 0, NBIN - 1), jax.random.fold_in(arg_keys[4], 1), 0, (NBIN - 1) - 1).astype(jnp.int32)
    arrival_fracs = jnp.clip(1.0 * jax.random.uniform(arg_keys[5], (TROWS, NOB, SP), jnp.float32) ** level_of(arg_keys[5], (TROWS, NOB, SP), ((0, 32),), -0.2, 0.2), 0.0, 1.0)
    gain_table = bell_draw_with(arg_keys[6], (TROWS, TERMS, NOB, OBS_BLOCK), TROWS ** -0.5, 0.125, ((0, 32),), (0, 3, 32, 2.75))
    return {"sources": sources, "owners": owners, "strip_rows": strip_rows, "panel_counts": panel_counts, "arrival_bins": arrival_bins, "arrival_fracs": arrival_fracs, "gain_table": gain_table}


def interp_weights(bin_ids, fractions):
    positions = jnp.arange(NBIN, dtype=jnp.int32)
    lower = jnp.where(positions[None, None, :] == bin_ids[:, :, None], 1.0 - fractions[:, :, None], 0.0)
    upper = jnp.where(positions[None, None, :] == bin_ids[:, :, None] + 1, fractions[:, :, None], 0.0)
    return (lower + upper).astype(jnp.bfloat16)


def reference(sources, owners, strip_rows, panel_counts, arrival_bins, arrival_fracs, gain_table):
    live_mask = (jnp.arange(SP, dtype=jnp.int32)[None, :] < panel_counts[:, None]).astype(jnp.float32)
    masked = sources.astype(jnp.float32) * live_mask[:, None, :]
    global_rows = (owners[:, 0] * ROWS + strip_rows).astype(jnp.int32)
    row_sources = jax.ops.segment_sum(masked, global_rows, num_segments=ROWS * N_GX)
    row_rounded = row_sources.astype(jnp.bfloat16)

    def patch_term(running, patch_index):
        first_row = (patch_index * ROWS).astype(jnp.int32)
        patch_sources = lax.dynamic_slice_in_dim(row_rounded, first_row, ROWS, 0).astype(jnp.float32)
        patch_bins = lax.dynamic_slice_in_dim(arrival_bins, first_row, ROWS, 0)
        patch_fracs = lax.dynamic_slice_in_dim(arrival_fracs, first_row, ROWS, 0)
        patch_gains = lax.dynamic_slice_in_dim(gain_table, first_row, ROWS, 0).astype(jnp.float32)
        for block_index in range(NOB):
            weights = interp_weights(patch_bins[:, block_index, :], patch_fracs[:, block_index, :]).astype(jnp.float32)
            arrived = jnp.einsum('rkp,rpb->rkb', patch_sources, weights, precision=lax.Precision.HIGHEST)
            arrived_rounded = arrived.astype(jnp.bfloat16).astype(jnp.float32)
            added = jnp.einsum('rkt,rkb->tb', patch_gains[:, :, block_index, :], arrived_rounded, precision=lax.Precision.HIGHEST)
            running = running.at[:, block_index, :].add(added)
        return running, None

    start_value = jnp.zeros((OBS_BLOCK, NOB, NBIN), jnp.float32)
    signals, unused = lax.scan(patch_term, start_value, jnp.arange(N_GX, dtype=jnp.int32))
    return signals
```

```python
import jax
import jax.numpy as jnp
from jax import lax
from jax.experimental import pallas as pl
from jax.experimental.pallas import tpu as pltpu
from jax.sharding import PartitionSpec as P

MESH = pl.DeviceIdType.MESH
F32 = jnp.float32
BF16 = jnp.bfloat16
I32 = jnp.int32

NX = 32
NZ = 4
ND = NX * NZ
STRIPS = 64
TERMS = 8
PANELS = 128
ROWS = 256
NBIN = 256
CAP = 4
TIMES = 1024
GROUP = 16
BLOCKS = ROWS // GROUP
NT = (((1,), (1,)), ((), ()))


def iota(shape, dim):
    return lax.broadcasted_iota(I32, shape, dim)


def dot(a, b):
    return jnp.dot(a, b, preferred_element_type=F32)


def dot_nt(a, b):
    return lax.dot_general(a, b, NT, preferred_element_type=F32)


def wait_all(ref, sem):
    block = ref.at[pl.ds(0, ND - 1)]
    pltpu.make_async_copy(block, block, sem).wait()


def kernel(
    src_ref, own_ref, row_ref, cnt_ref, bins_hbm, fracs_hbm, gains_hbm, out_ref,
    send_s, send_m, got_s, got_m, bins, fracs, gains, weights, rows, spread, arrived,
    send_p, got_p, in_sem, gain_sem, ss_sem, sm_sem, sp_sem, rs_sem, rm_sem, rp_sem,
):
    mx = lax.axis_index("gx")
    mz = lax.axis_index("gy")

    def gain_copy(tile):
        return pltpu.make_async_copy(gains_hbm.at[:, tile, mz // 2], gains.at[tile], gain_sem.at[tile])

    bins_copy = pltpu.make_async_copy(bins_hbm, bins, in_sem.at[0])
    fracs_copy = pltpu.make_async_copy(fracs_hbm, fracs, in_sem.at[1])
    bins_copy.start()
    fracs_copy.start()

    owner = own_ref[...]
    row1 = row_ref[...] + 1
    hot = (iota((NX, STRIPS), 0) == owner).astype(F32)
    upto = (iota((STRIPS, STRIPS), 0) <= iota((STRIPS, STRIPS), 1)).astype(F32).astype(BF16)
    seen = dot(hot.astype(BF16), upto)
    place = jnp.sum(hot * (seen - 1.0), axis=0, keepdims=True)
    slot = owner.astype(F32) * CAP + place
    lane_of = (iota((128, STRIPS), 0) == (place.astype(I32) + mx * CAP)).astype(F32).astype(BF16)
    meta = dot_nt((hot * row1.astype(F32)).astype(BF16), lane_of)
    for j in range(NX):
        send_m[j] = meta[j : j + 1, :]
    wide = (iota((STRIPS, STRIPS * TERMS), 0) == iota((STRIPS, STRIPS * TERMS), 1) >> 3)
    wide = wide.astype(F32).astype(BF16)
    slot_c = dot(jnp.broadcast_to(slot, (8, STRIPS)).astype(BF16), wide)[0:1].astype(I32)
    tall = (iota((STRIPS * TERMS, STRIPS), 1) == iota((STRIPS * TERMS, STRIPS), 0) >> 3)
    tall = tall.astype(F32).astype(BF16)
    count = dot_nt(tall, jnp.broadcast_to(cnt_ref[...].astype(F32), (128, STRIPS)).astype(BF16))
    live = iota((STRIPS * TERMS, PANELS), 1).astype(F32) < count
    masked = jnp.where(live, src_ref[...].astype(F32), 0.0).astype(BF16)
    term = iota((1, STRIPS * TERMS), 1) & 7
    for kk in range(4):
        dest = jnp.where((term & 3) == kk, 2 * slot_c + (term >> 2), -1)
        placing = (iota((ND * 2, STRIPS * TERMS), 0) == dest).astype(F32).astype(BF16)
        placed = dot(placing, masked)
        send_s[:, :, kk * 128 : (kk + 1) * 128] = placed.reshape(NX, 8, 128).astype(BF16)

    def strip_copy(j, z):
        return pltpu.make_async_remote_copy(
            src_ref=send_s.at[j], dst_ref=got_s.at[mz * NX + mx], send_sem=ss_sem, recv_sem=rs_sem,
            device_id={"gx": j, "gy": z}, device_id_type=MESH,
        )

    def meta_copy(j, z):
        return pltpu.make_async_remote_copy(
            src_ref=send_m.at[j], dst_ref=got_m.at[mz * NX + mx], send_sem=sm_sem, recv_sem=rm_sem,
            device_id={"gx": j, "gy": z}, device_id_type=MESH,
        )

    def peer(step):
        other = lax.rem(mx * NZ + mz + step, ND)
        return other // NZ, lax.rem(other, NZ)

    @pl.loop(1, ND)
    def _(step):
        j, z = peer(step)
        strip_copy(j, z).start()
        meta_copy(j, z).start()

    got_s[mz * NX + mx] = send_s[mx]
    got_m[mz * NX + mx] = send_m[mx]

    for tile in range(8):
        gain_copy(tile).start()

    bins_copy.wait()
    fracs_copy.wait()
    where_b = iota((NBIN, PANELS), 0).astype(F32).astype(BF16)

    @pl.loop(0, ROWS // 8)
    def _(step):
        start = step * 8 * NZ + mz
        low = bins[pl.ds(start, 8, stride=NZ), :].astype(F32)
        high = low + 1.0
        frac = fracs[pl.ds(start, 8, stride=NZ), :]
        rest = 1.0 - frac
        low, high, frac, rest = (x.astype(BF16) for x in (low, high, frac, rest))
        for i in range(8):
            pick = lambda x: jnp.broadcast_to(x[i : i + 1, :], (NBIN, PANELS))
            value = jnp.where(where_b == pick(high), pick(frac), jnp.zeros((), BF16))
            value = jnp.where(where_b == pick(low), pick(rest), value)
            lanes = pl.ds(pl.multiple_of((step * 8 + i) * PANELS, PANELS), PANELS)
            weights[:, lanes] = value

    spread[...] = jnp.zeros_like(spread)

    wait_all(got_s, rs_sem)
    wait_all(got_m, rm_sem)

    half = iota((1, 2 * ND), 1) & 1
    twice = (iota((128, 2 * 128), 0) == iota((128, 2 * 128), 1) >> 1).astype(F32).astype(BF16)
    sums = [jnp.zeros((ROWS, 512), F32) for _ in range(2)]
    for z in range(NZ):
        row_of = jnp.sum(got_m[z * NX : (z + 1) * NX].reshape(NX, 128), axis=0, keepdims=True)
        row_of = dot(jnp.broadcast_to(row_of, (8, 128)).astype(BF16), twice)[0:1].astype(I32) - 1
        data = got_s[z * NX : (z + 1) * NX].reshape(NX * 8, 512)
        for h in range(2):
            hit = (iota((ROWS, 2 * 128), 0) == jnp.where(half == h, row_of, -1)).astype(F32).astype(BF16)
            sums[h] = sums[h] + dot(hit, data)
    even = lax.rem(mz, 2) == 0
    for k in range(TERMS):
        value = sums[k // 4][:, (k % 4) * 128 : (k % 4 + 1) * 128]
        rows[pl.ds(2 * k, ROWS, stride=16), :] = jnp.where(even, value, 0.0)
        rows[pl.ds(2 * k + 1, ROWS, stride=16), :] = jnp.where(even, 0.0, value)

    lane_row = iota((PANELS, 128), 1) >> 4

    @pl.loop(0, BLOCKS)
    def _(blk):
        part = rows[pl.ds(pl.multiple_of(blk * 256, 256), 256), :]
        flat = part.astype(BF16).astype(F32).T
        for g in range(GROUP):
            tile = g // 8
            piece = jnp.where(lane_row == g % 8, flat[:, tile * 128 : (tile + 1) * 128], 0.0)
            spread[g * PANELS : (g + 1) * PANELS, tile * 128 : (tile + 1) * 128] = piece.astype(BF16)
        lanes = pl.ds(pl.multiple_of(blk * GROUP * PANELS, GROUP * PANELS), GROUP * PANELS)
        value = dot(weights[:, lanes], spread[...])
        arrived[:, pl.ds(pl.multiple_of(blk * 256, 256), 256)] = value.astype(BF16)

    def part_copy(q):
        j, z = q // NZ, lax.rem(q, NZ)
        return pltpu.make_async_remote_copy(
            src_ref=send_p.at[q], dst_ref=got_p.at[mz * NX + mx], send_sem=sp_sem, recv_sem=rp_sem,
            device_id={"gx": j, "gy": z}, device_id_type=MESH,
        )

    me = mx * NZ + mz
    for turn in range(4):
        n = lax.rem(mx // 8 + turn, 4)
        for i in range(2):
            gain_copy(2 * n + i).wait()
        pair = [gains.at[2 * n + i].reshape(ROWS * TERMS * 2, 128)[...] for i in range(2)]
        value = dot(arrived[...], jnp.concatenate(pair, axis=1)).T
        send_p[pl.ds(n * 32, 32)] = value.reshape(32, 8, NBIN).astype(BF16)

        @pl.loop(0, 32)
        def _(step):
            q = n * 32 + lax.rem(me + step, 32)

            @pl.when(q != me)
            def _():
                part_copy(q).start()

    got_p[mz * NX + mx] = send_p[me]
    wait_all(got_p, rp_sem)
    for o in range(NZ):
        total = jnp.zeros((8, NBIN), F32)
        for i in range(NX):
            total = total + got_p[o * NX + i].astype(F32)
        out_ref[o] = total

    wait_all(got_s, ss_sem)
    wait_all(got_m, sm_sem)
    wait_all(got_p, sp_sem)


def on_device(sources, owners, strip_rows, panel_counts, arrival_bins, arrival_fracs, gain_table):
    any_space = pl.BlockSpec(memory_space=pl.ANY)
    vmem = pl.BlockSpec(memory_space=pltpu.VMEM)
    gains = gain_table.reshape(ROWS * TERMS, NZ, 8, 128).transpose(0, 2, 1, 3)
    gains = gains.reshape(ROWS * TERMS, 8, 2, 2, 128)
    dma = pltpu.SemaphoreType.DMA
    out = pl.pallas_call(
        kernel,
        out_shape=jax.ShapeDtypeStruct((NZ, 8, NBIN), F32),
        in_specs=[vmem, vmem, vmem, vmem, any_space, any_space, any_space],
        out_specs=vmem,
        scratch_shapes=[
            pltpu.VMEM((NX, 8, 512), BF16),
            pltpu.VMEM((NX, 1, 128), F32),
            pltpu.VMEM((ND, 8, 512), BF16),
            pltpu.VMEM((ND, 1, 128), F32),
            pltpu.VMEM((ROWS * NZ, PANELS), I32),
            pltpu.VMEM((ROWS * NZ, PANELS), F32),
            pltpu.VMEM((8, ROWS * TERMS, 2, 128), BF16),
            pltpu.VMEM((NBIN, ROWS * PANELS), BF16),
            pltpu.VMEM((ROWS * TERMS * 2, PANELS), F32),
            pltpu.VMEM((GROUP * PANELS, 256), BF16),
            pltpu.VMEM((NBIN, ROWS * TERMS * 2), BF16),
            pltpu.VMEM((ND, 8, NBIN), BF16),
            pltpu.VMEM((ND, 8, NBIN), BF16),
            dma((2,)), dma((8,)),
            dma, dma, dma, dma, dma, dma,
        ],
        compiler_params=pltpu.CompilerParams(
            has_side_effects=True, vmem_limit_bytes=60 * 1024 * 1024
        ),
    )(
        sources.reshape(STRIPS * TERMS, PANELS),
        owners.reshape(1, STRIPS),
        strip_rows.reshape(1, STRIPS),
        panel_counts.reshape(1, STRIPS),
        arrival_bins.reshape(ROWS * NZ, PANELS),
        arrival_fracs.reshape(ROWS * NZ, PANELS),
        gains,
    )
    return out.transpose(1, 0, 2)


def solution(mesh):
    placed = (
        P(("gx", "gy"), None, None),
        P(("gx", "gy"), None),
        P(("gx", "gy")),
        P(("gx", "gy")),
        P("gx", None, None),
        P("gx", None, None),
        P("gx", None, None, None),
    )
    return jax.shard_map(
        on_device,
        mesh=mesh,
        in_specs=placed,
        out_specs=P(("gx", "gy"), None, None),
        check_vma=False,
    )
```

```python
import jax
import jax.numpy as jnp
from jax import lax
from jax.experimental import pallas as pl
from jax.experimental.pallas import tpu as pltpu
from jax.sharding import PartitionSpec as P

MESH = pl.DeviceIdType.MESH
F32 = jnp.float32
BF16 = jnp.bfloat16
I32 = jnp.int32

NX = 32
NZ = 4
ND = NX * NZ
STRIPS = 64
TERMS = 8
PANELS = 128
ROWS = 256
NBIN = 256
CAP = 4
TIMES = 1024
GROUP = 16
BLOCKS = ROWS // GROUP
UNROLL = 4
NT = (((1,), (1,)), ((), ()))


def iota(shape, dim):
    return lax.broadcasted_iota(I32, shape, dim)


def dot(a, b):
    return jnp.dot(a, b, preferred_element_type=F32)


def dot_nt(a, b):
    return lax.dot_general(a, b, NT, preferred_element_type=F32)


SIDES = (0, 1, 3, 2)


def wait_bytes(ref, blocks, sem):
    block = ref.at[pl.ds(0, blocks)]
    pltpu.make_async_copy(block, block, sem).wait()


def kernel(
    src_ref, own_ref, row_ref, cnt_ref, bins_hbm, fracs_hbm, gains_hbm, out_ref,
    send_s, send_m, got_s, got_m, bins, fracs, gains, weights, rows, spread, arrived,
    row_at, send_p, got_p, in_sem, gain_sem, ss_sem, sm_sem, sp_sem, rs_sem, rm_sem, rp_sem,
    zs_sem, zr_sem, za_sem, zb_sem, ms_sem, mr_sem,
):
    mx = lax.axis_index("gx")
    mz = lax.axis_index("gy")
    scopes = []

    def phase(name=None):
        if scopes:
            scopes.pop().__exit__(None, None, None)
        if name:
            scopes.append(jax.named_scope(name))
            scopes[-1].__enter__()

    def gain_copy(tile):
        return pltpu.make_async_copy(gains_hbm.at[:, tile, mz // 2], gains.at[tile], gain_sem.at[tile])

    bins_copy = pltpu.make_async_copy(bins_hbm, bins, in_sem.at[0])
    fracs_copy = pltpu.make_async_copy(fracs_hbm, fracs, in_sem.at[1])
    bins_copy.start()
    fracs_copy.start()
    for tile in range(8):
        gain_copy(tile).start()

    barrier = pltpu.get_barrier_semaphore()
    up, down, across = (lax.rem(mz + i, NZ) for i in (1, 3, 2))

    @pl.loop(1, NX)
    def _(step):
        peer = lax.rem(mx + step, NX)
        pl.semaphore_signal(barrier, inc=1, device_id={"gx": peer, "gy": mz}, device_id_type=MESH)

    for peer in (up, down, across):
        pl.semaphore_signal(barrier, inc=1, device_id={"gx": mx, "gy": peer}, device_id_type=MESH)

    def weigh(first, last):
        where_b = iota((NBIN, PANELS), 0).astype(F32).astype(BF16)

        @pl.loop(first, last)
        def _(step):
            start = step * 8 * NZ + mz
            low = bins[pl.ds(start, 8, stride=NZ), :].astype(F32)
            high = low + 1.0
            frac = fracs[pl.ds(start, 8, stride=NZ), :]
            rest = 1.0 - frac
            low, high, frac, rest = (x.astype(BF16) for x in (low, high, frac, rest))
            for i in range(8):
                pick = lambda x: jnp.broadcast_to(x[i : i + 1, :], (NBIN, PANELS))
                value = jnp.where(where_b == pick(high), pick(frac), jnp.zeros((), BF16))
                value = jnp.where(where_b == pick(low), pick(rest), value)
                lanes = pl.ds(pl.multiple_of((step * 8 + i) * PANELS, PANELS), PANELS)
                weights[:, lanes] = value

    phase("prep")
    owner = own_ref[...]
    row1 = row_ref[...] + 1
    hot = (iota((NX, STRIPS), 0) == owner).astype(F32)
    upto = (iota((STRIPS, STRIPS), 0) <= iota((STRIPS, STRIPS), 1)).astype(F32).astype(BF16)
    seen = dot(hot.astype(BF16), upto)
    place = jnp.sum(hot * (seen - 1.0), axis=0, keepdims=True)
    slot = owner.astype(F32) * CAP + place
    lane_of = (iota((128, STRIPS), 0) == (place.astype(I32) + mx * CAP)).astype(F32).astype(BF16)
    meta = dot_nt((hot * row1.astype(F32)).astype(BF16), lane_of)
    for j in range(NX):
        send_m[j] = meta[j : j + 1, :]
    wide = (iota((STRIPS, STRIPS * TERMS), 0) == iota((STRIPS, STRIPS * TERMS), 1) >> 3)
    wide = wide.astype(F32).astype(BF16)
    slot_c = dot(jnp.broadcast_to(slot, (8, STRIPS)).astype(BF16), wide)[0:1].astype(I32)
    tall = (iota((STRIPS * TERMS, STRIPS), 1) == iota((STRIPS * TERMS, STRIPS), 0) >> 3)
    tall = tall.astype(F32).astype(BF16)
    count = dot_nt(tall, jnp.broadcast_to(cnt_ref[...].astype(F32), (128, STRIPS)).astype(BF16))
    live = iota((STRIPS * TERMS, PANELS), 1).astype(F32) < count
    masked = jnp.where(live, src_ref[...].astype(F32), 0.0).astype(BF16)
    term = iota((1, STRIPS * TERMS), 1) & 7
    for kk in range(4):
        dest = jnp.where((term & 3) == kk, 2 * slot_c + (term >> 2), -1)
        placing = (iota((ND * 2, STRIPS * TERMS), 0) == dest).astype(F32).astype(BF16)
        placed = dot(placing, masked)
        send_s[:, :, kk * 128 : (kk + 1) * 128] = placed.reshape(NX, 8, 128).astype(BF16)

    phase("barrier")
    pl.semaphore_wait(barrier, NX - 1 + NZ - 1)

    my = mx // 8

    def strip_copy(j, side):
        return pltpu.make_async_remote_copy(
            src_ref=send_s.at[j], dst_ref=got_s.at[mz * NX + mx], send_sem=ss_sem,
            recv_sem=rs_sem.at[side], device_id={"gx": j, "gy": mz}, device_id_type=MESH,
        )

    def meta_copy(j):
        return pltpu.make_async_remote_copy(
            src_ref=send_m.at[j], dst_ref=got_m.at[mx], send_sem=sm_sem, recv_sem=rm_sem,
            device_id={"gx": j, "gy": mz}, device_id_type=MESH,
        )

    phase("send")
    for side in SIDES:
        for i in range(8):
            j = lax.rem(my + NZ - side, 4) * 8 + lax.rem(mx + i, 8)
            if side or i:
                strip_copy(j, side).start()

    @pl.loop(1, NX)
    def _(step):
        meta_copy(lax.rem(mx + step, NX)).start()

    got_s[mz * NX + mx] = send_s[mx]
    got_m[mx] = send_m[mx]

    def group(z, side, half=None):
        first = z * NX + lax.rem(my + side, 4) * 8
        if half is None:
            return got_s.at[pl.ds(first, 8)]
        return got_s.at[pl.ds(first + half * 4, 4)]

    def ring_copy(side, way):
        block = group(mz, side)
        return pltpu.make_async_remote_copy(
            src_ref=block, dst_ref=block, send_sem=zs_sem.at[way, side],
            recv_sem=zr_sem.at[way, side], device_id={"gx": mx, "gy": (up, down)[way]},
            device_id_type=MESH,
        )

    def relay_copy(side, way):
        block = group((down, up)[way], side, way)
        return pltpu.make_async_remote_copy(
            src_ref=block, dst_ref=block, send_sem=za_sem.at[way, side],
            recv_sem=zb_sem.at[way, side], device_id={"gx": mx, "gy": (up, down)[way]},
            device_id_type=MESH,
        )

    def weigh_some(count):
        first = done[0]
        done[0] = min(first + count, ROWS // 8)
        if done[0] > first:
            phase("weights")
            weigh(first, done[0])

    done = [0]
    bins_copy.wait()
    fracs_copy.wait()
    weigh_some(8)
    for side in SIDES:
        phase("near")
        wait_bytes(got_s, 8 if side else 7, rs_sem.at[side])
        for way in range(2):
            ring_copy(side, way).start()
        weigh_some(2)
    phase("meta")
    wait_bytes(got_m, NX - 1, rm_sem)
    row_at[mz] = jnp.sum(got_m[...].reshape(NX, 128), axis=0, keepdims=True)

    def row_copy(i):
        peer = (up, down, across)[i]
        return pltpu.make_async_remote_copy(
            src_ref=row_at.at[mz], dst_ref=row_at.at[mz], send_sem=ms_sem.at[i],
            recv_sem=mr_sem.at[i], device_id={"gx": mx, "gy": peer}, device_id_type=MESH,
        )

    for i in range(3):
        row_copy(i).start()
    for side in SIDES:
        weigh_some(4)
        phase("relay")
        for way in range(2):
            ring_copy(side, way).wait_recv()
            relay_copy(side, way).start()
    weigh_some(ROWS)
    phase("clear")
    spread[...] = jnp.zeros_like(spread)
    phase("arrive")
    for i in range(3):
        row_copy(i).wait_recv()
    for side in SIDES:
        for way in range(2):
            relay_copy(side, way).wait_recv()

    phase("sums")
    half = iota((1, 2 * ND), 1) & 1
    twice = (iota((128, 2 * 128), 0) == iota((128, 2 * 128), 1) >> 1).astype(F32).astype(BF16)
    sums = [jnp.zeros((ROWS, 512), F32) for _ in range(2)]
    for z in range(NZ):
        row_of = dot(jnp.broadcast_to(row_at[z], (8, 128)).astype(BF16), twice)[0:1].astype(I32) - 1
        data = got_s[z * NX : (z + 1) * NX].reshape(NX * 8, 512)
        for h in range(2):
            hit = (iota((ROWS, 2 * 128), 0) == jnp.where(half == h, row_of, -1)).astype(F32).astype(BF16)
            sums[h] = sums[h] + dot(hit, data)
    even = lax.rem(mz, 2) == 0
    for k in range(TERMS):
        value = sums[k // 4][:, (k % 4) * 128 : (k % 4 + 1) * 128]
        rows[pl.ds(2 * k, ROWS, stride=16), :] = jnp.where(even, value, 0.0)
        rows[pl.ds(2 * k + 1, ROWS, stride=16), :] = jnp.where(even, 0.0, value)

    phase('binning')
    lane_row = iota((PANELS, 128), 1) >> 4

    @pl.loop(0, BLOCKS // UNROLL)
    def _(turn):
        for u in range(UNROLL):
            blk = turn * UNROLL + u
            part = rows[pl.ds(pl.multiple_of(blk * 256, 256), 256), :]
            flat = part.astype(BF16).astype(F32).T
            for g in range(GROUP):
                tile = g // 8
                piece = jnp.where(lane_row == g % 8, flat[:, tile * 128 : (tile + 1) * 128], 0.0)
                spread[u, g * PANELS : (g + 1) * PANELS, tile * 128 : (tile + 1) * 128] = piece.astype(BF16)
            lanes = pl.ds(pl.multiple_of(blk * GROUP * PANELS, GROUP * PANELS), GROUP * PANELS)
            value = dot(weights[:, lanes], spread[u])
            arrived[:, pl.ds(pl.multiple_of(blk * 256, 256), 256)] = value.astype(BF16)

    def part_copy(q):
        j, z = q // NZ, lax.rem(q, NZ)
        return pltpu.make_async_remote_copy(
            src_ref=send_p.at[q], dst_ref=got_p.at[mz * NX + mx], send_sem=sp_sem, recv_sem=rp_sem,
            device_id={"gx": j, "gy": z}, device_id_type=MESH,
        )

    phase("signals")
    me = mx * NZ + mz
    for tile in range(8):
        gain_copy(tile).wait()

    def times_of(side):
        n = lax.rem(my + side, 4)
        pair = [gains.at[2 * n + i].reshape(ROWS * TERMS * 2, 128)[...] for i in range(2)]
        return dot(arrived[...], jnp.concatenate(pair, axis=1))

    def send_times(side, value):
        n = lax.rem(my + side, 4)
        send_p[pl.ds(n * 32, 32)] = value.T.reshape(32, 8, NBIN).astype(BF16)
        for step in range(0 if side else 1, 32):
            part_copy(n * 32 + lax.rem(me + step, 32)).start()

    order = (2, 1, 3, 0)
    value = times_of(order[0])
    for i in range(4):
        following = times_of(order[i + 1]) if i < 3 else None
        send_times(order[i], value)
        value = following

    phase("collect")
    got_p[mz * NX + mx] = send_p[me]
    wait_bytes(got_p, ND - 1, rp_sem)
    phase("total")
    for o in range(NZ):
        total = jnp.zeros((8, NBIN), F32)
        for i in range(NX):
            total = total + got_p[o * NX + i].astype(F32)
        out_ref[o] = total
    phase("drain")
    wait_bytes(got_s, NX - 1, ss_sem)
    wait_bytes(got_m, NX - 1, sm_sem)
    wait_bytes(got_p, ND - 1, sp_sem)
    for i in range(3):
        row_copy(i).wait_send()
    for side in SIDES:
        for way in range(2):
            ring_copy(side, way).wait_send()
            relay_copy(side, way).wait_send()
    phase()


def on_device(sources, owners, strip_rows, panel_counts, arrival_bins, arrival_fracs, gain_table):
    any_space = pl.BlockSpec(memory_space=pl.ANY)
    vmem = pl.BlockSpec(memory_space=pltpu.VMEM)
    gains = gain_table.reshape(ROWS * TERMS, NZ, 8, 128).transpose(0, 2, 1, 3)
    gains = gains.reshape(ROWS * TERMS, 8, 2, 2, 128)
    dma = pltpu.SemaphoreType.DMA
    out = pl.pallas_call(
        kernel,
        out_shape=jax.ShapeDtypeStruct((NZ, 8, NBIN), F32),
        in_specs=[vmem, vmem, vmem, vmem, any_space, any_space, any_space],
        out_specs=vmem,
        scratch_shapes=[
            pltpu.VMEM((NX, 8, 512), BF16),
            pltpu.VMEM((NX, 1, 128), F32),
            pltpu.VMEM((ND, 8, 512), BF16),
            pltpu.VMEM((NX, 1, 128), F32),
            pltpu.VMEM((ROWS * NZ, PANELS), I32),
            pltpu.VMEM((ROWS * NZ, PANELS), F32),
            pltpu.VMEM((8, ROWS * TERMS, 2, 128), BF16),
            pltpu.VMEM((NBIN, ROWS * PANELS), BF16),
            pltpu.VMEM((ROWS * TERMS * 2, PANELS), F32),
            pltpu.VMEM((UNROLL, GROUP * PANELS, 256), BF16),
            pltpu.VMEM((NBIN, ROWS * TERMS * 2), BF16),
            pltpu.VMEM((NZ, 1, 128), F32),
            pltpu.VMEM((ND, 8, NBIN), BF16),
            pltpu.VMEM((ND, 8, NBIN), BF16),
            dma((2,)), dma((8,)), dma, dma, dma, dma((4,)), dma, dma,
            dma((2, 4)), dma((2, 4)), dma((2, 4)), dma((2, 4)), dma((3,)), dma((3,)),
        ],
        compiler_params=pltpu.CompilerParams(
            collective_id=0, has_side_effects=True, vmem_limit_bytes=60 * 1024 * 1024
        ),
    )(
        sources.reshape(STRIPS * TERMS, PANELS),
        owners.reshape(1, STRIPS),
        strip_rows.reshape(1, STRIPS),
        panel_counts.reshape(1, STRIPS),
        arrival_bins.reshape(ROWS * NZ, PANELS),
        arrival_fracs.reshape(ROWS * NZ, PANELS),
        gains,
    )
    return out.transpose(1, 0, 2)


def solution(mesh):
    placed = (
        P(("gx", "gy"), None, None),
        P(("gx", "gy"), None),
        P(("gx", "gy")),
        P(("gx", "gy")),
        P("gx", None, None),
        P("gx", None, None),
        P("gx", None, None, None),
    )
    return jax.shard_map(
        on_device,
        mesh=mesh,
        in_specs=placed,
        out_specs=P(("gx", "gy"), None, None),
        check_vma=False,
    )
```

```python
import jax
import jax.numpy as jnp
from jax import lax
from jax.experimental import pallas as pl
from jax.experimental.pallas import tpu as pltpu
from jax.sharding import PartitionSpec as P

MESH = pl.DeviceIdType.MESH
F32 = jnp.float32
BF16 = jnp.bfloat16
I32 = jnp.int32

NX = 32
NZ = 4
ND = NX * NZ
STRIPS = 64
TERMS = 8
PANELS = 128
ROWS = 256
NBIN = 256
CAP = 4
TIMES = 1024
HALF = NBIN // 2
TALL = HALF + 16
UNROLL = 4
NT = (((1,), (1,)), ((), ()))


def iota(shape, dim):
    return lax.broadcasted_iota(I32, shape, dim)


def dot(a, b):
    return jnp.dot(a, b, preferred_element_type=F32)


def dot_nt(a, b):
    return lax.dot_general(a, b, NT, preferred_element_type=F32)


SIDES = (0, 1, 3, 2)
DIRECT = ()


def wait_bytes(ref, blocks, sem):
    block = ref.at[pl.ds(0, blocks)]
    pltpu.make_async_copy(block, block, sem).wait()


def kernel(
    src_hbm, own_hbm, row_hbm, cnt_hbm, bins_hbm, fracs_hbm, gains_hbm, out_ref,
    send_s, send_m, got_s, got_m, bins, fracs, gains, weights, rows, arrived,
    chosen, select, sums, row_at, send_q, got_q, send_p, got_p, in_sem, gain_sem, ss_sem, sm_sem, sp_sem, rs_sem, rm_sem, rp_sem,
    zs_sem, zr_sem, za_sem, zb_sem, ms_sem, mr_sem, qs_sem, qr_sem, ds_sem,
    src_ref, own_ref, row_ref, cnt_ref,
):
    mx = lax.axis_index("gx")
    mz = lax.axis_index("gy")
    scopes = []

    def phase(name=None):
        if scopes:
            scopes.pop().__exit__(None, None, None)
        if name:
            scopes.append(jax.named_scope(name))
            scopes[-1].__enter__()

    def gain_copy(tile):
        return pltpu.make_async_copy(gains_hbm.at[:, tile, mz // 2], gains.at[tile], gain_sem.at[tile])

    barrier = pltpu.get_barrier_semaphore()
    up, down, across = (lax.rem(mz + i, NZ) for i in (1, 3, 2))

    @pl.loop(1, NX)
    def _(step):
        peer = lax.rem(mx + step, NX)
        pl.semaphore_signal(barrier, inc=1, device_id={"gx": peer, "gy": mz}, device_id_type=MESH)

    pl.semaphore_signal(barrier, inc=1, device_id={"gx": mx, "gy": across}, device_id_type=MESH)

    if not DIRECT:
        for plane in (up, down):
            pl.semaphore_signal(barrier, inc=1, device_id={"gx": mx, "gy": plane}, device_id_type=MESH)

    @pl.loop(0, 8 * len(DIRECT))
    def _(step):
        peer = (mx // 8 * 8 + step // 8 * 8 + lax.rem(mx + step, 8)) & (NX - 1)
        for plane in (up, down):
            pl.semaphore_signal(barrier, inc=1, device_id={"gx": peer, "gy": plane}, device_id_type=MESH)

    small = [
        pltpu.make_async_copy(hbm, ref, in_sem.at[2 + i])
        for i, (hbm, ref) in enumerate(
            ((own_hbm, own_ref), (row_hbm, row_ref), (cnt_hbm, cnt_ref), (src_hbm, src_ref))
        )
    ]
    for copy in small:
        copy.start()
    bins_copy = pltpu.make_async_copy(bins_hbm, bins, in_sem.at[0])
    fracs_copy = pltpu.make_async_copy(fracs_hbm, fracs, in_sem.at[1])
    bins_copy.start()
    fracs_copy.start()

    def weigh(first, last):
        where_b = iota((TALL, PANELS), 0).astype(F32).astype(BF16)

        @pl.loop(first, last)
        def _(step):
            start = step * 8 * NZ + mz
            low = (bins[pl.ds(start, 8, stride=NZ), :] & (HALF - 1)).astype(F32)
            high = low + 1.0
            frac = fracs[pl.ds(start, 8, stride=NZ), :]
            rest = 1.0 - frac
            low, high, frac, rest = (x.astype(BF16) for x in (low, high, frac, rest))
            for i in range(8):
                pick = lambda x: jnp.broadcast_to(x[i : i + 1, :], (TALL, PANELS))
                value = jnp.where(where_b == pick(high), pick(frac), jnp.zeros((), BF16))
                value = jnp.where(where_b == pick(low), pick(rest), value)
                weights[step * 8 + i] = value

    phase("prep")
    for copy in small:
        copy.wait()
    owner = own_ref[...]
    row1 = row_ref[...] + 1
    hot = (iota((NX, STRIPS), 0) == owner).astype(F32)
    upto = (iota((STRIPS, STRIPS), 0) <= iota((STRIPS, STRIPS), 1)).astype(F32).astype(BF16)
    seen = dot(hot.astype(BF16), upto)
    place = jnp.sum(hot * (seen - 1.0), axis=0, keepdims=True)
    slot = owner.astype(F32) * CAP + place
    lane_of = (iota((128, STRIPS), 0) == (place.astype(I32) + mx * CAP)).astype(F32).astype(BF16)
    meta = dot_nt((hot * row1.astype(F32)).astype(BF16), lane_of)
    for j in range(NX):
        send_m[j] = meta[j : j + 1, :]
    wide = (iota((STRIPS, STRIPS * TERMS), 0) == iota((STRIPS, STRIPS * TERMS), 1) >> 3)
    wide = wide.astype(F32).astype(BF16)
    slot_c = dot(jnp.broadcast_to(slot, (8, STRIPS)).astype(BF16), wide)[0:1].astype(I32)
    tall = (iota((STRIPS * TERMS, STRIPS), 1) == iota((STRIPS * TERMS, STRIPS), 0) >> 3)
    tall = tall.astype(F32).astype(BF16)
    count = dot_nt(tall, jnp.broadcast_to(cnt_ref[...].astype(F32), (128, STRIPS)).astype(BF16))
    live = iota((STRIPS * TERMS, PANELS), 1).astype(F32) < count
    masked = jnp.where(live, src_ref[...].astype(F32), 0.0).astype(BF16)
    term = iota((1, STRIPS * TERMS), 1) & 7
    for kk in range(4):
        dest = jnp.where((term & 3) == kk, 2 * slot_c + (term >> 2), -1)
        placing = (iota((ND * 2, STRIPS * TERMS), 0) == dest).astype(F32).astype(BF16)
        placed = dot(placing, masked)
        send_s[:, :, kk * 128 : (kk + 1) * 128] = placed.reshape(NX, 8, 128).astype(BF16)

    phase("barrier")
    pl.semaphore_wait(barrier, NX + (16 * len(DIRECT) or 2))

    my = mx // 8

    def strip_copy(j, side):
        return pltpu.make_async_remote_copy(
            src_ref=send_s.at[j], dst_ref=got_s.at[mz * NX + mx], send_sem=ss_sem,
            recv_sem=rs_sem.at[side], device_id={"gx": j, "gy": mz}, device_id_type=MESH,
        )

    def meta_copy(j):
        return pltpu.make_async_remote_copy(
            src_ref=send_m.at[j], dst_ref=got_m.at[mx], send_sem=sm_sem, recv_sem=rm_sem,
            device_id={"gx": j, "gy": mz}, device_id_type=MESH,
        )

    def direct_copy(j, side, way):
        return pltpu.make_async_remote_copy(
            src_ref=send_s.at[j], dst_ref=got_s.at[mz * NX + mx], send_sem=ds_sem,
            recv_sem=zr_sem.at[way, side], device_id={"gx": j, "gy": (up, down)[way]},
            device_id_type=MESH,
        )

    phase("send")
    for side in SIDES:
        for i in range(8):
            j = lax.rem(my + NZ - side, 4) * 8 + lax.rem(mx + i, 8)
            if side or i:
                strip_copy(j, side).start()
    @pl.loop(1, NX)
    def _(step):
        meta_copy(lax.rem(mx + step, NX)).start()

    for side in DIRECT:
        for i in range(8):
            j = lax.rem(my + NZ - side, 4) * 8 + lax.rem(mx + i, 8)
            for way in range(2):
                direct_copy(j, side, way).start()

    for tile in range(8):
        gain_copy(tile).start()
    got_s[mz * NX + mx] = send_s[mx]
    got_m[mx] = send_m[mx]

    def group(z, side, half=None):
        first = z * NX + lax.rem(my + side, 4) * 8
        if half is None:
            return got_s.at[pl.ds(first, 8)]
        return got_s.at[pl.ds(first + half * 4, 4)]

    def ring_copy(side, way):
        block = group(mz, side)
        return pltpu.make_async_remote_copy(
            src_ref=block, dst_ref=block, send_sem=zs_sem.at[way, side],
            recv_sem=zr_sem.at[way, side], device_id={"gx": mx, "gy": (up, down)[way]},
            device_id_type=MESH,
        )

    def relay_copy(side, way):
        block = group((down, up)[way], side, way)
        return pltpu.make_async_remote_copy(
            src_ref=block, dst_ref=block, send_sem=za_sem.at[way, side],
            recv_sem=zb_sem.at[way, side], device_id={"gx": mx, "gy": (up, down)[way]},
            device_id_type=MESH,
        )

    def weigh_some(count):
        first = done[0]
        done[0] = min(first + count, ROWS // 8)
        if done[0] > first:
            phase("weights")
            weigh(first, done[0])

    def choose_some(count):
        first = done[1]
        done[1] = min(first + count, 8)
        if done[1] == first:
            return
        phase("choose")

        @pl.loop(first, done[1])
        def _(step):
            n = step // 2
            for u in range(8):
                at = lax.rem(step, 2) * 8 + u
                taken = pl.ds(pl.multiple_of(at * 256, 256), 256)
                pair = [gains.at[2 * n + i].reshape(ROWS * TERMS * 2, 128)[taken, :] for i in range(2)]
                value = dot(select[...], jnp.concatenate(pair, axis=1))
                for i in range(2):
                    half = value[:, i * 128 : (i + 1) * 128].astype(BF16)
                    chosen[2 * n + i, pl.ds(pl.multiple_of(at * 128, 128), 128), :] = half

    done = [0, 0]
    select[...] = (
        iota((128, 256), 1) == 2 * iota((128, 256), 0) + lax.rem(mz, 2)
    ).astype(F32).astype(BF16)
    bins_copy.wait()
    fracs_copy.wait()
    weigh_some(ROWS)
    for i, side in enumerate(SIDES):
        phase("near")
        wait_bytes(got_s, 8 if side else 7, rs_sem.at[side])
        for way in range(0 if side in DIRECT else 2):
            ring_copy(side, way).start()
        if i == 0:
            for tile in range(8):
                gain_copy(tile).wait()
        choose_some(1)
    phase("meta")
    wait_bytes(got_m, NX - 1, rm_sem)
    row_at[mz] = jnp.sum(got_m[...].reshape(NX, 128), axis=0, keepdims=True)

    def row_copy(i):
        peer = (up, down, across)[i]
        return pltpu.make_async_remote_copy(
            src_ref=row_at.at[mz], dst_ref=row_at.at[mz], send_sem=ms_sem.at[i],
            recv_sem=mr_sem.at[i], device_id={"gx": mx, "gy": peer}, device_id_type=MESH,
        )

    for i in range(3):
        row_copy(i).start()

    half = iota((1, 2 * ND), 1) & 1
    twice = (iota((128, 2 * 128), 0) == iota((128, 2 * 128), 1) >> 1).astype(F32).astype(BF16)

    def plane_sums(z):
        row_of = dot(jnp.broadcast_to(row_at[z], (8, 128)).astype(BF16), twice)[0:1].astype(I32) - 1
        data = got_s[pl.ds(z * NX, NX)].reshape(NX * 8, 512)
        parts = []
        for h in range(2):
            hit = (iota((ROWS, 2 * 128), 0) == jnp.where(half == h, row_of, -1)).astype(F32).astype(BF16)
            parts.append(dot(hit, data))
        return parts

    def add_plane(z, first):
        phase("plane")
        for h, part in enumerate(plane_sums(z)):
            lanes = slice(h * 512, (h + 1) * 512)
            sums[:, lanes] = part if first else sums[:, lanes] + part

    for i, side in enumerate(SIDES):
        if i == 1:
            add_plane(mz, True)
        choose_some(1)
        phase("relay")
        for way in range(2):
            ring_copy(side, way).wait_recv()
            relay_copy(side, way).start()
    for i in range(2):
        phase("rows")
        row_copy(i).wait_recv()
        add_plane((down, up)[i], False)
    choose_some(8)
    phase("arrive")
    row_copy(2).wait_recv()
    for side in SIDES:
        for way in range(2):
            relay_copy(side, way).wait_recv()

    phase("sums")
    for h, part in enumerate(plane_sums(across)):
        part = part + sums[:, h * 512 : (h + 1) * 512]
        for k in range(4):
            rows[pl.ds(h * 4 + k, ROWS, stride=TERMS), :] = part[:, k * 128 : (k + 1) * 128]

    phase("binning")
    lane_row = (iota((PANELS, 128), 1) >> 3).astype(F32).astype(BF16)

    @pl.loop(0, ROWS // 16 // UNROLL)
    def _(turn):
        for u in range(UNROLL):
            group = turn * UNROLL + u
            part = rows[pl.ds(pl.multiple_of(group * 128, 128), 128), :].astype(BF16).astype(F32)
            high = bins[pl.ds(group * 16 * NZ + mz, 16, stride=NZ), :] >> 7
            high = [jnp.broadcast_to(high[g : g + 1, :], (TERMS, PANELS)) for g in range(16)]
            zero = jnp.where(jnp.concatenate(high, axis=0) == 0, part, 0.0)
            flats = [flat.T.astype(BF16) for flat in (zero, part - zero)]
            zeros = jnp.zeros((), BF16)
            wide = [
                jnp.concatenate([jnp.where(lane_row == g, flat, zeros) for flat in flats], axis=1)
                for g in range(16)
            ]
            tall = jnp.concatenate([weights[group * 16 + g] for g in range(16)], axis=1)
            value = dot(tall, jnp.concatenate(wide, axis=0))
            low, high = value[0:HALF, 0:128], value[0:HALF, 128:256]
            carried = high[0:8] + value[HALF : HALF + 8, 0:128]
            arrived[group, 0:HALF, :] = low.astype(BF16)
            arrived[group, HALF:NBIN, :] = jnp.concatenate([carried, high[8:]], axis=0).astype(BF16)

    phase("signals")
    core = lax.rem(mx, 2)
    chip_x = (mx // 2) & 3
    sibling = mx + 1 - 2 * core
    near_half = chip_x >> 1

    def tiles_of(c):
        sides = (2, 1 + 2 * c, 3 - 2 * c, 0)
        halves = (1 - c, 1, 0, 1 - c)
        return [((my + side) & 3, (near_half + half) & 1) for side, half in zip(sides, halves)]

    theirs, mine = tiles_of(1 - core), tiles_of(core)

    def times_of(tiles):
        tall = jnp.concatenate([arrived[group] for group in range(16)], axis=1)
        value = dot(tall, jnp.concatenate([chosen[2 * y + half] for y, half in tiles], axis=1))
        return [value[:, i * 256 : (i + 1) * 256].T.reshape(32, 8, NBIN) for i in range(2)]

    def pair_copy(i):
        return pltpu.make_async_remote_copy(
            src_ref=send_q.at[i], dst_ref=got_q.at[i], send_sem=qs_sem.at[i], recv_sem=qr_sem.at[i],
            device_id={"gx": sibling, "gy": mz}, device_id_type=MESH,
        )

    def part_copy(tile, dx, dz, dc):
        y, half = mine[tile]
        x, c, z = ((chip_x + dx) & 1) + 2 * half, (core + dc) & 1, (mz + dz) & 3
        return pltpu.make_async_remote_copy(
            src_ref=send_p.at[tile, ((x & 1) * 2 + c) * NZ + z], dst_ref=got_p.at[mz * 16 + mx // 2],
            send_sem=sp_sem, recv_sem=rp_sem,
            device_id={"gx": y * 8 + x * 2 + c, "gy": z}, device_id_type=MESH,
        )

    for i, value in enumerate(times_of(theirs)):
        send_q[i] = value.astype(BF16)
        pair_copy(i).start()
    for i, value in enumerate(times_of(mine)):
        pair_copy(i).wait_recv()
        value = (value + got_q[i].astype(F32)).astype(BF16)
        for tile in (2 * i, 2 * i + 1):
            send_p[tile] = value[(tile & 1) * 16 : (tile & 1) * 16 + 16]
            for dz in (2, 1, 3, 0):
                for dx in (1, 0):
                    for dc in (1, 0):
                        if tile < 3 or dx or dz or dc:
                            part_copy(tile, dx, dz, dc).start()

    phase("collect")
    keeps = core == 1

    @pl.when(keeps)
    def _():
        got_p[mz * 16 + mx // 2] = send_p[3, ((chip_x & 1) * 2 + core) * NZ + mz]
        wait_bytes(got_p, 63, rp_sem)
        wait_bytes(got_p, 63, sp_sem)

    @pl.when(jnp.logical_not(keeps))
    def _():
        part_copy(3, 0, 0, 0).start()
        wait_bytes(got_p, 64, rp_sem)
        wait_bytes(got_p, 64, sp_sem)

    phase("total")
    for o in range(NZ):
        total = jnp.zeros((8, NBIN), F32)
        for i in range(16):
            total = total + got_p[o * 16 + i].astype(F32)
        out_ref[o] = total
    phase("drain")
    wait_bytes(got_s, NX - 1, ss_sem)
    wait_bytes(got_m, NX - 1, sm_sem)
    if DIRECT:
        wait_bytes(got_s, 16 * len(DIRECT), ds_sem)
    for i in range(2):
        pair_copy(i).wait_send()
    for i in range(3):
        row_copy(i).wait_send()
    for side in SIDES:
        for way in range(2):
            if side not in DIRECT:
                ring_copy(side, way).wait_send()
            relay_copy(side, way).wait_send()
    phase()


def on_device(sources, owners, strip_rows, panel_counts, arrival_bins, arrival_fracs, gain_table):
    any_space = pl.BlockSpec(memory_space=pl.ANY)
    vmem = pl.BlockSpec(memory_space=pltpu.VMEM)
    gains = gain_table.reshape(ROWS * TERMS, NZ, 8, 128).transpose(0, 2, 1, 3)
    gains = gains.reshape(ROWS * TERMS, 8, 2, 2, 128)
    dma = pltpu.SemaphoreType.DMA
    out = pl.pallas_call(
        kernel,
        out_shape=pltpu.VMEM((NZ, 8, NBIN), F32),
        in_specs=[any_space] * 7,
        out_specs=vmem,
        scratch_shapes=[
            pltpu.VMEM((NX, 8, 512), BF16),
            pltpu.VMEM((NX, 1, 128), F32),
            pltpu.VMEM((ND, 8, 512), BF16),
            pltpu.VMEM((NX, 1, 128), F32),
            pltpu.VMEM((ROWS * NZ, PANELS), I32),
            pltpu.VMEM((ROWS * NZ, PANELS), F32),
            pltpu.VMEM((8, ROWS * TERMS, 2, 128), BF16),
            pltpu.VMEM((ROWS, TALL, PANELS), BF16),
            pltpu.VMEM((ROWS * TERMS, PANELS), F32),
            pltpu.VMEM((16, NBIN, 128), BF16),
            pltpu.VMEM((8, ROWS * TERMS, 128), BF16),
            pltpu.VMEM((128, 256), BF16),
            pltpu.VMEM((ROWS, TERMS * PANELS), F32),
            pltpu.VMEM((NZ, 1, 128), F32),
            pltpu.VMEM((2, 32, 8, NBIN), BF16),
            pltpu.VMEM((2, 32, 8, NBIN), BF16),
            pltpu.VMEM((4, 16, 8, NBIN), BF16),
            pltpu.VMEM((64, 8, NBIN), BF16),
            dma((6,)), dma((8,)), dma, dma, dma, dma((4,)), dma, dma,
            dma((2, 4)), dma((2, 4)), dma((2, 4)), dma((2, 4)), dma((3,)), dma((3,)), dma((2,)), dma((2,)), dma,
            pltpu.VMEM((STRIPS * TERMS, PANELS), BF16),
            pltpu.VMEM((1, STRIPS), I32), pltpu.VMEM((1, STRIPS), I32), pltpu.VMEM((1, STRIPS), I32),
        ],
        compiler_params=pltpu.CompilerParams(
            collective_id=0, has_side_effects=True, vmem_limit_bytes=60 * 1024 * 1024
        ),
    )(
        sources.reshape(STRIPS * TERMS, PANELS),
        owners.reshape(1, STRIPS),
        strip_rows.reshape(1, STRIPS),
        panel_counts.reshape(1, STRIPS),
        arrival_bins.reshape(ROWS * NZ, PANELS),
        arrival_fracs.reshape(ROWS * NZ, PANELS),
        gains,
    )
    return out.transpose(1, 0, 2)


def solution(mesh):
    placed = (
        P(("gx", "gy"), None, None),
        P(("gx", "gy"), None),
        P(("gx", "gy")),
        P(("gx", "gy")),
        P("gx", None, None),
        P("gx", None, None),
        P("gx", None, None, None),
    )
    return jax.shard_map(
        on_device,
        mesh=mesh,
        in_specs=placed,
        out_specs=P(("gx", "gy"), None, None),
        check_vma=False,
    )
```

```python
import jax
import jax.numpy as jnp
from jax import lax
from jax.experimental import pallas as pl
from jax.experimental.pallas import tpu as pltpu
from jax.sharding import PartitionSpec as P

MESH = pl.DeviceIdType.MESH
F32 = jnp.float32
BF16 = jnp.bfloat16
I32 = jnp.int32

NX = 32
NZ = 4
ND = NX * NZ
STRIPS = 64
TERMS = 8
PANELS = 128
ROWS = 256
NBIN = 256
CAP = 4
TIMES = 1024
HALF = NBIN // 2
TALL = HALF + 16
NT = (((1,), (1,)), ((), ()))


def iota(shape, dim):
    return lax.broadcasted_iota(I32, shape, dim)


def dot(a, b):
    return jnp.dot(a, b, preferred_element_type=F32)


def dot_nt(a, b):
    return lax.dot_general(a, b, NT, preferred_element_type=F32)


SIDES = (0, 1, 3, 2)
DIRECT = ()


def wait_bytes(ref, blocks, sem):
    block = ref.at[pl.ds(0, blocks)]
    pltpu.make_async_copy(block, block, sem).wait()


def kernel(
    src_hbm, own_hbm, row_hbm, cnt_hbm, bins_hbm, fracs_hbm, gains_hbm, out_ref,
    send_s, send_m, got_s, got_m, bins, fracs, gains, weights, rows, arrived,
    chosen, select, sums, row_at, send_q, got_q, send_p, got_p, in_sem, gain_sem, ss_sem, sm_sem, sp_sem, rs_sem, rm_sem, rp_sem,
    zs_sem, zr_sem, za_sem, zb_sem, ms_sem, mr_sem, qs_sem, qr_sem, ds_sem,
    src_ref, own_ref, row_ref, cnt_ref,
):
    mx = lax.axis_index("gx")
    mz = lax.axis_index("gy")
    scopes = []

    def phase(name=None):
        if scopes:
            scopes.pop().__exit__(None, None, None)
        if name:
            scopes.append(jax.named_scope(name))
            scopes[-1].__enter__()

    def gain_copy(tile):
        return pltpu.make_async_copy(gains_hbm.at[:, tile, mz // 2], gains.at[tile], gain_sem.at[tile])

    small = [
        pltpu.make_async_copy(hbm, ref, in_sem.at[2 + i])
        for i, (hbm, ref) in enumerate(
            ((own_hbm, own_ref), (row_hbm, row_ref), (cnt_hbm, cnt_ref), (src_hbm, src_ref))
        )
    ]
    for copy in small:
        copy.start()
    bins_copy = pltpu.make_async_copy(bins_hbm, bins, in_sem.at[0])
    fracs_copy = pltpu.make_async_copy(fracs_hbm, fracs, in_sem.at[1])
    bins_copy.start()
    fracs_copy.start()

    barrier = pltpu.get_barrier_semaphore()
    up, down, across = (lax.rem(mz + i, NZ) for i in (1, 3, 2))

    @pl.loop(1, NX)
    def _(step):
        peer = lax.rem(mx + step, NX)
        pl.semaphore_signal(barrier, inc=1, device_id={"gx": peer, "gy": mz}, device_id_type=MESH)

    pl.semaphore_signal(barrier, inc=1, device_id={"gx": mx, "gy": across}, device_id_type=MESH)

    if not DIRECT:
        for plane in (up, down):
            pl.semaphore_signal(barrier, inc=1, device_id={"gx": mx, "gy": plane}, device_id_type=MESH)

    @pl.loop(0, 8 * len(DIRECT))
    def _(step):
        peer = (mx // 8 * 8 + step // 8 * 8 + lax.rem(mx + step, 8)) & (NX - 1)
        for plane in (up, down):
            pl.semaphore_signal(barrier, inc=1, device_id={"gx": peer, "gy": plane}, device_id_type=MESH)

    def weigh(first, last):
        where_b = iota((TALL, PANELS), 0).astype(F32).astype(BF16)

        @pl.loop(first, last)
        def _(step):
            start = step * 8 * NZ + mz
            low = (bins[pl.ds(start, 8, stride=NZ), :] & (HALF - 1)).astype(F32)
            high = low + 1.0
            frac = fracs[pl.ds(start, 8, stride=NZ), :]
            rest = 1.0 - frac
            low, high, frac, rest = (x.astype(BF16) for x in (low, high, frac, rest))
            for i in range(8):
                pick = lambda x: jnp.broadcast_to(x[i : i + 1, :], (TALL, PANELS))
                value = jnp.where(where_b == pick(high), pick(frac), jnp.zeros((), BF16))
                value = jnp.where(where_b == pick(low), pick(rest), value)
                weights[step * 8 + i] = value

    phase("prep")
    for copy in small:
        copy.wait()
    owner = own_ref[...]
    row1 = row_ref[...] + 1
    hot = (iota((NX, STRIPS), 0) == owner).astype(F32)
    upto = (iota((STRIPS, STRIPS), 0) <= iota((STRIPS, STRIPS), 1)).astype(F32).astype(BF16)
    seen = dot(hot.astype(BF16), upto)
    place = jnp.sum(hot * (seen - 1.0), axis=0, keepdims=True)
    slot = owner.astype(F32) * CAP + place
    lane_of = (iota((128, STRIPS), 0) == (place.astype(I32) + mx * CAP)).astype(F32).astype(BF16)
    meta = dot_nt((hot * row1.astype(F32)).astype(BF16), lane_of)
    for j in range(NX):
        send_m[j] = meta[j : j + 1, :]
    wide = (iota((STRIPS, STRIPS * TERMS), 0) == iota((STRIPS, STRIPS * TERMS), 1) >> 3)
    wide = wide.astype(F32).astype(BF16)
    slot_c = dot(jnp.broadcast_to(slot, (8, STRIPS)).astype(BF16), wide)[0:1].astype(I32)
    tall = (iota((STRIPS * TERMS, STRIPS), 1) == iota((STRIPS * TERMS, STRIPS), 0) >> 3)
    tall = tall.astype(F32).astype(BF16)
    count = dot_nt(tall, jnp.broadcast_to(cnt_ref[...].astype(F32), (128, STRIPS)).astype(BF16))
    live = iota((STRIPS * TERMS, PANELS), 1).astype(F32) < count
    masked = jnp.where(live, src_ref[...].astype(F32), 0.0).astype(BF16)
    term = iota((1, STRIPS * TERMS), 1) & 7
    slot_rows = iota((ND * 2, STRIPS * TERMS), 0).astype(F32).astype(BF16)
    for kk in range(4):
        dest = jnp.where((term & 3) == kk, 2 * slot_c + (term >> 2), -1).astype(F32).astype(BF16)
        placing = jnp.where(slot_rows == dest, jnp.ones((), BF16), jnp.zeros((), BF16))
        placed = dot(placing, masked)
        send_s[:, :, kk * 128 : (kk + 1) * 128] = placed.reshape(NX, 8, 128).astype(BF16)

    phase("barrier")
    pl.semaphore_wait(barrier, NX + (16 * len(DIRECT) or 2))

    my = mx // 8

    def strip_copy(j, side):
        return pltpu.make_async_remote_copy(
            src_ref=send_s.at[j], dst_ref=got_s.at[mz * NX + mx], send_sem=ss_sem,
            recv_sem=rs_sem.at[side], device_id={"gx": j, "gy": mz}, device_id_type=MESH,
        )

    def meta_copy(j):
        return pltpu.make_async_remote_copy(
            src_ref=send_m.at[j], dst_ref=got_m.at[mx], send_sem=sm_sem, recv_sem=rm_sem,
            device_id={"gx": j, "gy": mz}, device_id_type=MESH,
        )

    def direct_copy(j, side, way):
        return pltpu.make_async_remote_copy(
            src_ref=send_s.at[j], dst_ref=got_s.at[mz * NX + mx], send_sem=ds_sem,
            recv_sem=zr_sem.at[way, side], device_id={"gx": j, "gy": (up, down)[way]},
            device_id_type=MESH,
        )

    phase("send")
    for side in SIDES:
        for i in range(8):
            j = lax.rem(my + NZ - side, 4) * 8 + lax.rem(mx + i, 8)
            if side or i:
                strip_copy(j, side).start()
    @pl.loop(1, NX)
    def _(step):
        meta_copy(lax.rem(mx + step, NX)).start()

    for side in DIRECT:
        for i in range(8):
            j = lax.rem(my + NZ - side, 4) * 8 + lax.rem(mx + i, 8)
            for way in range(2):
                direct_copy(j, side, way).start()

    for tile in range(8):
        gain_copy(tile).start()
    got_s[mz * NX + mx] = send_s[mx]
    got_m[mx] = send_m[mx]

    def group(z, side, half=None):
        first = z * NX + lax.rem(my + side, 4) * 8
        if half is None:
            return got_s.at[pl.ds(first, 8)]
        return got_s.at[pl.ds(first + half * 4, 4)]

    def ring_copy(side, way):
        block = group(mz, side)
        return pltpu.make_async_remote_copy(
            src_ref=block, dst_ref=block, send_sem=zs_sem.at[way, side],
            recv_sem=zr_sem.at[way, side], device_id={"gx": mx, "gy": (up, down)[way]},
            device_id_type=MESH,
        )

    def relay_copy(side, way):
        block = group((down, up)[way], side, way)
        return pltpu.make_async_remote_copy(
            src_ref=block, dst_ref=block, send_sem=za_sem.at[way, side],
            recv_sem=zb_sem.at[way, side], device_id={"gx": mx, "gy": (up, down)[way]},
            device_id_type=MESH,
        )

    def weigh_some(count):
        first = done[0]
        done[0] = min(first + count, ROWS // 8)
        if done[0] > first:
            phase("weights")
            weigh(first, done[0])

    def choose_some(count):
        first = done[1]
        done[1] = min(first + count, 8)
        if done[1] == first:
            return
        phase("choose")

        @pl.loop(first, done[1])
        def _(step):
            n = step // 2
            for u in range(8):
                at = lax.rem(step, 2) * 8 + u
                taken = pl.ds(pl.multiple_of(at * 256, 256), 256)
                pair = [gains.at[2 * n + i].reshape(ROWS * TERMS * 2, 128)[taken, :] for i in range(2)]
                value = dot(select[...], jnp.concatenate(pair, axis=1))
                for i in range(2):
                    half = value[:, i * 128 : (i + 1) * 128].astype(BF16)
                    chosen[2 * n + i, pl.ds(pl.multiple_of(at * 128, 128), 128), :] = half

    done = [0, 0]
    select[...] = (
        iota((128, 256), 1) == 2 * iota((128, 256), 0) + lax.rem(mz, 2)
    ).astype(F32).astype(BF16)
    bins_copy.wait()
    fracs_copy.wait()
    weigh_some(ROWS)
    for i, side in enumerate(SIDES):
        phase("near")
        wait_bytes(got_s, 8 if side else 7, rs_sem.at[side])
        for way in range(0 if side in DIRECT else 2):
            ring_copy(side, way).start()
        if i == 0:
            for tile in range(8):
                gain_copy(tile).wait()
        choose_some(1)
    phase("meta")
    wait_bytes(got_m, NX - 1, rm_sem)
    row_at[mz] = jnp.sum(got_m[...].reshape(NX, 128), axis=0, keepdims=True)

    def row_copy(i):
        peer = (up, down, across)[i]
        return pltpu.make_async_remote_copy(
            src_ref=row_at.at[mz], dst_ref=row_at.at[mz], send_sem=ms_sem.at[i],
            recv_sem=mr_sem.at[i], device_id={"gx": mx, "gy": peer}, device_id_type=MESH,
        )

    for i in range(3):
        row_copy(i).start()

    half = iota((1, 2 * ND), 1) & 1
    twice = (iota((128, 2 * 128), 0) == iota((128, 2 * 128), 1) >> 1).astype(F32).astype(BF16)

    row_ids = iota((ROWS, 2 * 128), 0).astype(F32).astype(BF16)

    def plane_hits(z):
        row_of = dot(jnp.broadcast_to(row_at[z], (8, 128)).astype(BF16), twice)[0:1] - 1.0
        hits = [jnp.where(half == h, row_of, -1.0).astype(BF16) for h in range(2)]
        return [jnp.where(row_ids == hit, jnp.ones((), BF16), jnp.zeros((), BF16)) for hit in hits]

    def plane_sums(z, hits):
        data = got_s[pl.ds(z * NX, NX)].reshape(NX * 8, 512)
        return [dot(hit, data) for hit in hits]

    def add_plane(z, first):
        phase("plane")
        for h, part in enumerate(plane_sums(z, plane_hits(z))):
            lanes = slice(h * 512, (h + 1) * 512)
            sums[:, lanes] = part if first else sums[:, lanes] + part

    for i, side in enumerate(SIDES):
        if i == 1:
            add_plane(mz, True)
        choose_some(1)
        phase("relay")
        for way in range(2):
            ring_copy(side, way).wait_recv()
            relay_copy(side, way).start()
    for i in range(2):
        phase("rows")
        row_copy(i).wait_recv()
        add_plane((down, up)[i], False)
    choose_some(8)
    phase("arrive")
    row_copy(2).wait_recv()
    last_hits = plane_hits(across)
    for side in SIDES:
        for way in range(2):
            relay_copy(side, way).wait_recv()

    phase("sums")
    for h, part in enumerate(plane_sums(across, last_hits)):
        part = part + sums[:, h * 512 : (h + 1) * 512]
        for k in range(4):
            rows[pl.ds(h * 4 + k, ROWS, stride=TERMS), :] = part[:, k * 128 : (k + 1) * 128]

    phase("binning")
    lane_row = (iota((PANELS, 128), 1) >> 3).astype(F32).astype(BF16)

    for batch in range(ROWS // 16):
        part = rows[batch * 128 : (batch + 1) * 128, :].astype(BF16).astype(F32)
        high = bins[pl.ds(batch * 16 * NZ + mz, 16, stride=NZ), :] >> 7
        high = [jnp.broadcast_to(high[g : g + 1, :], (TERMS, PANELS)) for g in range(16)]
        zero = jnp.where(jnp.concatenate(high, axis=0) == 0, part, 0.0)
        flats = [flat.T.astype(BF16) for flat in (zero, part - zero)]
        zeros = jnp.zeros((), BF16)
        wide = [
            jnp.concatenate([jnp.where(lane_row == g, flat, zeros) for flat in flats], axis=1)
            for g in range(16)
        ]
        tall = jnp.concatenate([weights[batch * 16 + g] for g in range(16)], axis=1)
        value = dot(tall, jnp.concatenate(wide, axis=0))
        low, high = value[0:HALF, 0:128], value[0:HALF, 128:256]
        carried = high[0:8] + value[HALF : HALF + 8, 0:128]
        arrived[batch, 0:HALF, :] = low.astype(BF16)
        arrived[batch, HALF:NBIN, :] = jnp.concatenate([carried, high[8:]], axis=0).astype(BF16)

    phase("signals")
    core = lax.rem(mx, 2)
    chip_x = (mx // 2) & 3
    sibling = mx + 1 - 2 * core
    near_half = chip_x >> 1

    def tiles_of(c):
        sides = (2, 1 + 2 * c, 3 - 2 * c, 0)
        halves = (1 - c, 1, 0, 1 - c)
        return [((my + side) & 3, (near_half + half) & 1) for side, half in zip(sides, halves)]

    theirs, mine = tiles_of(1 - core), tiles_of(core)

    def times_of(tiles):
        tall = jnp.concatenate([arrived[group] for group in range(16)], axis=1)
        value = dot(tall, jnp.concatenate([chosen[2 * y + half] for y, half in tiles], axis=1))
        return [value[:, i * 256 : (i + 1) * 256].T.reshape(32, 8, NBIN) for i in range(2)]

    def pair_copy(i):
        return pltpu.make_async_remote_copy(
            src_ref=send_q.at[i], dst_ref=got_q.at[i], send_sem=qs_sem.at[i], recv_sem=qr_sem.at[i],
            device_id={"gx": sibling, "gy": mz}, device_id_type=MESH,
        )

    def part_copy(tile, dx, dz, dc):
        y, half = mine[tile]
        x, c, z = ((chip_x + dx) & 1) + 2 * half, (core + dc) & 1, (mz + dz) & 3
        return pltpu.make_async_remote_copy(
            src_ref=send_p.at[tile, ((x & 1) * 2 + c) * NZ + z], dst_ref=got_p.at[mz * 16 + mx // 2],
            send_sem=sp_sem, recv_sem=rp_sem,
            device_id={"gx": y * 8 + x * 2 + c, "gy": z}, device_id_type=MESH,
        )

    for i, value in enumerate(times_of(theirs)):
        send_q[i] = value.astype(BF16)
        pair_copy(i).start()
    for i, value in enumerate(times_of(mine)):
        pair_copy(i).wait_recv()
        value = (value + got_q[i].astype(F32)).astype(BF16)
        for tile in (2 * i, 2 * i + 1):
            send_p[tile] = value[(tile & 1) * 16 : (tile & 1) * 16 + 16]
            for dz in (2, 1, 3, 0):
                for dx in (1, 0):
                    for dc in (1, 0):
                        if tile < 3 or dx or dz or dc:
                            part_copy(tile, dx, dz, dc).start()

    phase("collect")
    keeps = core == 1

    @pl.when(keeps)
    def _():
        got_p[mz * 16 + mx // 2] = send_p[3, ((chip_x & 1) * 2 + core) * NZ + mz]
        wait_bytes(got_p, 63, rp_sem)
        wait_bytes(got_p, 63, sp_sem)

    @pl.when(jnp.logical_not(keeps))
    def _():
        part_copy(3, 0, 0, 0).start()
        wait_bytes(got_p, 64, rp_sem)
        wait_bytes(got_p, 64, sp_sem)

    phase("total")
    for o in range(NZ):
        total = jnp.zeros((8, NBIN), F32)
        for i in range(16):
            total = total + got_p[o * 16 + i].astype(F32)
        out_ref[o] = total
    phase("drain")
    wait_bytes(got_s, NX - 1, ss_sem)
    wait_bytes(got_m, NX - 1, sm_sem)
    if DIRECT:
        wait_bytes(got_s, 16 * len(DIRECT), ds_sem)
    for i in range(2):
        pair_copy(i).wait_send()
    for i in range(3):
        row_copy(i).wait_send()
    for side in SIDES:
        for way in range(2):
            if side not in DIRECT:
                ring_copy(side, way).wait_send()
            relay_copy(side, way).wait_send()
    phase()


def on_device(sources, owners, strip_rows, panel_counts, arrival_bins, arrival_fracs, gain_table):
    any_space = pl.BlockSpec(memory_space=pl.ANY)
    vmem = pl.BlockSpec(memory_space=pltpu.VMEM)
    gains = gain_table.reshape(ROWS * TERMS, NZ, 8, 128).transpose(0, 2, 1, 3)
    gains = gains.reshape(ROWS * TERMS, 8, 2, 2, 128)
    dma = pltpu.SemaphoreType.DMA
    out = pl.pallas_call(
        kernel,
        out_shape=pltpu.VMEM((NZ, 8, NBIN), F32),
        in_specs=[any_space] * 7,
        out_specs=vmem,
        scratch_shapes=[
            pltpu.VMEM((NX, 8, 512), BF16),
            pltpu.VMEM((NX, 1, 128), F32),
            pltpu.VMEM((ND, 8, 512), BF16),
            pltpu.VMEM((NX, 1, 128), F32),
            pltpu.VMEM((ROWS * NZ, PANELS), I32),
            pltpu.VMEM((ROWS * NZ, PANELS), F32),
            pltpu.VMEM((8, ROWS * TERMS, 2, 128), BF16),
            pltpu.VMEM((ROWS, TALL, PANELS), BF16),
            pltpu.VMEM((ROWS * TERMS, PANELS), F32),
            pltpu.VMEM((16, NBIN, 128), BF16),
            pltpu.VMEM((8, ROWS * TERMS, 128), BF16),
            pltpu.VMEM((128, 256), BF16),
            pltpu.VMEM((ROWS, TERMS * PANELS), F32),
            pltpu.VMEM((NZ, 1, 128), F32),
            pltpu.VMEM((2, 32, 8, NBIN), BF16),
            pltpu.VMEM((2, 32, 8, NBIN), BF16),
            pltpu.VMEM((4, 16, 8, NBIN), BF16),
            pltpu.VMEM((64, 8, NBIN), BF16),
            dma((6,)), dma((8,)), dma, dma, dma, dma((4,)), dma, dma,
            dma((2, 4)), dma((2, 4)), dma((2, 4)), dma((2, 4)), dma((3,)), dma((3,)), dma((2,)), dma((2,)), dma,
            pltpu.VMEM((STRIPS * TERMS, PANELS), BF16),
            pltpu.VMEM((1, STRIPS), I32), pltpu.VMEM((1, STRIPS), I32), pltpu.VMEM((1, STRIPS), I32),
        ],
        compiler_params=pltpu.CompilerParams(
            collective_id=0, has_side_effects=True, vmem_limit_bytes=60 * 1024 * 1024
        ),
    )(
        sources.reshape(STRIPS * TERMS, PANELS),
        owners.reshape(1, STRIPS),
        strip_rows.reshape(1, STRIPS),
        panel_counts.reshape(1, STRIPS),
        arrival_bins.reshape(ROWS * NZ, PANELS),
        arrival_fracs.reshape(ROWS * NZ, PANELS),
        gains,
    )
    return out.transpose(1, 0, 2)


def solution(mesh):
    placed = (
        P(("gx", "gy"), None, None),
        P(("gx", "gy"), None),
        P(("gx", "gy")),
        P(("gx", "gy")),
        P("gx", None, None),
        P("gx", None, None),
        P("gx", None, None, None),
    )
    return jax.shard_map(
        on_device,
        mesh=mesh,
        in_specs=placed,
        out_specs=P(("gx", "gy"), None, None),
        check_vma=False,
    )
```

```python
import jax
import jax.numpy as jnp
from jax import lax
from jax.experimental import pallas as pl
from jax.experimental.pallas import tpu as pltpu
from jax.sharding import PartitionSpec as P

MESH = pl.DeviceIdType.MESH
F32 = jnp.float32
BF16 = jnp.bfloat16
I32 = jnp.int32

NX = 32
NZ = 4
ND = NX * NZ
STRIPS = 64
TERMS = 8
PANELS = 128
ROWS = 256
NBIN = 256
CAP = 4
TIMES = 1024
HALF = NBIN // 2
TALL = HALF + 16
NT = (((1,), (1,)), ((), ()))


def iota(shape, dim):
    return lax.broadcasted_iota(I32, shape, dim)


def dot(a, b):
    return jnp.dot(a, b, preferred_element_type=F32)


def dot_nt(a, b):
    return lax.dot_general(a, b, NT, preferred_element_type=F32)


SIDES = (0, 1, 3, 2)


def wait_bytes(ref, blocks, sem):
    block = ref.at[pl.ds(0, blocks)]
    pltpu.make_async_copy(block, block, sem).wait()


def kernel(
    src_hbm, own_hbm, row_hbm, cnt_hbm, bins_hbm, fracs_hbm, gains_hbm, out_ref,
    send_s, send_m, got_s, got_m, bins, fracs, gains, weights, rows, arrived,
    chosen, select, sums, row_at, send_q, got_q, send_p, got_p, in_sem, gain_sem, ss_sem, sm_sem, sp_sem, rs_sem, rm_sem, rp_sem,
    zr_sem, zb_sem, ms_sem, mr_sem, qs_sem, qr_sem,
    src_ref, own_ref, row_ref, cnt_ref,
):
    mx = lax.axis_index("gx")
    mz = lax.axis_index("gy")
    scopes = []

    def phase(name=None):
        if scopes:
            scopes.pop().__exit__(None, None, None)
        if name:
            scopes.append(jax.named_scope(name))
            scopes[-1].__enter__()

    def gain_copy(tile):
        return pltpu.make_async_copy(gains_hbm.at[:, tile, mz // 2], gains.at[tile], gain_sem)

    small = [
        pltpu.make_async_copy(hbm, ref, in_sem.at[2 + i])
        for i, (hbm, ref) in enumerate(
            ((own_hbm, own_ref), (row_hbm, row_ref), (cnt_hbm, cnt_ref), (src_hbm, src_ref))
        )
    ]
    for copy in small:
        copy.start()
    bins_copy = pltpu.make_async_copy(bins_hbm, bins, in_sem.at[0])
    fracs_copy = pltpu.make_async_copy(fracs_hbm, fracs, in_sem.at[1])
    bins_copy.start()
    fracs_copy.start()

    barrier = pltpu.get_barrier_semaphore()
    up, down, across = (lax.rem(mz + i, NZ) for i in (1, 3, 2))

    @pl.loop(1, NX)
    def _(step):
        peer = lax.rem(mx + step, NX)
        pl.semaphore_signal(barrier, inc=1, device_id={"gx": peer, "gy": mz}, device_id_type=MESH)

    pl.semaphore_signal(barrier, inc=1, device_id={"gx": mx, "gy": across}, device_id_type=MESH)

    for plane in (up, down):
        pl.semaphore_signal(barrier, inc=1, device_id={"gx": mx, "gy": plane}, device_id_type=MESH)

    def weigh(first, last):
        where_b = iota((TALL, PANELS), 0).astype(F32).astype(BF16)

        @pl.loop(first, last)
        def _(step):
            start = step * 8 * NZ + mz
            low = (bins[pl.ds(start, 8, stride=NZ), :] & (HALF - 1)).astype(F32)
            high = low + 1.0
            frac = fracs[pl.ds(start, 8, stride=NZ), :]
            rest = 1.0 - frac
            low, high, frac, rest = (x.astype(BF16) for x in (low, high, frac, rest))
            for i in range(8):
                pick = lambda x: jnp.broadcast_to(x[i : i + 1, :], (TALL, PANELS))
                value = jnp.where(where_b == pick(high), pick(frac), jnp.zeros((), BF16))
                value = jnp.where(where_b == pick(low), pick(rest), value)
                weights[step * 8 + i] = value

    phase("prep")
    for copy in small:
        copy.wait()
    owner = own_ref[...]
    row1 = row_ref[...] + 1
    hot = (iota((NX, STRIPS), 0) == owner).astype(F32)
    upto = (iota((STRIPS, STRIPS), 0) <= iota((STRIPS, STRIPS), 1)).astype(F32).astype(BF16)
    seen = dot(hot.astype(BF16), upto)
    place = jnp.sum(hot * (seen - 1.0), axis=0, keepdims=True)
    slot = owner.astype(F32) * CAP + place
    lane_of = (iota((128, STRIPS), 0) == (place.astype(I32) + mx * CAP)).astype(F32).astype(BF16)
    meta = dot_nt((hot * row1.astype(F32)).astype(BF16), lane_of)
    for j in range(NX):
        send_m[j] = meta[j : j + 1, :]
    wide = (iota((STRIPS, STRIPS * TERMS), 0) == iota((STRIPS, STRIPS * TERMS), 1) >> 3)
    wide = wide.astype(F32).astype(BF16)
    slot_c = dot(jnp.broadcast_to(slot, (8, STRIPS)).astype(BF16), wide)[0:1].astype(I32)
    tall = (iota((STRIPS * TERMS, STRIPS), 1) == iota((STRIPS * TERMS, STRIPS), 0) >> 3)
    tall = tall.astype(F32).astype(BF16)
    count = dot_nt(tall, jnp.broadcast_to(cnt_ref[...].astype(F32), (128, STRIPS)).astype(BF16))
    live = iota((STRIPS * TERMS, PANELS), 1).astype(F32) < count
    masked = jnp.where(live, src_ref[...].astype(F32), 0.0).astype(BF16)
    term = iota((1, STRIPS * TERMS), 1) & 7
    slot_rows = iota((ND * 2, STRIPS * TERMS), 0).astype(F32).astype(BF16)
    for kk in range(4):
        dest = jnp.where((term & 3) == kk, 2 * slot_c + (term >> 2), -1).astype(F32).astype(BF16)
        placing = jnp.where(slot_rows == dest, jnp.ones((), BF16), jnp.zeros((), BF16))
        placed = dot(placing, masked)
        send_s[:, :, kk * 128 : (kk + 1) * 128] = placed.reshape(NX, 8, 128).astype(BF16)

    phase("barrier")
    pl.semaphore_wait(barrier, NX - 1 + NZ - 1)

    my = mx // 8

    def strip_copy(j, side):
        return pltpu.make_async_remote_copy(
            src_ref=send_s.at[j], dst_ref=got_s.at[mz * NX + mx], send_sem=ss_sem,
            recv_sem=rs_sem.at[side], device_id={"gx": j, "gy": mz}, device_id_type=MESH,
        )

    def meta_copy(j):
        return pltpu.make_async_remote_copy(
            src_ref=send_m.at[j], dst_ref=got_m.at[mx], send_sem=sm_sem, recv_sem=rm_sem,
            device_id={"gx": j, "gy": mz}, device_id_type=MESH,
        )

    phase("send")
    for side in SIDES:
        for i in range(8):
            j = lax.rem(my + NZ - side, 4) * 8 + lax.rem(mx + i, 8)
            if side or i:
                strip_copy(j, side).start()
    @pl.loop(1, NX)
    def _(step):
        meta_copy(lax.rem(mx + step, NX)).start()

    for tile in range(8):
        gain_copy(tile).start()
    got_s[mz * NX + mx] = send_s[mx]
    got_m[mx] = send_m[mx]

    def group(z, side, half=None):
        first = z * NX + lax.rem(my + side, 4) * 8
        if half is None:
            return got_s.at[pl.ds(first, 8)]
        return got_s.at[pl.ds(first + half * 4, 4)]

    def ring_copy(side, way):
        block = group(mz, side)
        return pltpu.make_async_remote_copy(
            src_ref=block, dst_ref=block, send_sem=ss_sem,
            recv_sem=zr_sem.at[way, side], device_id={"gx": mx, "gy": (up, down)[way]},
            device_id_type=MESH,
        )

    def relay_copy(side, way):
        block = group((down, up)[way], side, way)
        return pltpu.make_async_remote_copy(
            src_ref=block, dst_ref=block, send_sem=ss_sem,
            recv_sem=zb_sem, device_id={"gx": mx, "gy": (up, down)[way]},
            device_id_type=MESH,
        )

    def weigh_some(count):
        first = done[0]
        done[0] = min(first + count, ROWS // 8)
        if done[0] > first:
            phase("weights")
            weigh(first, done[0])

    def choose_some(count):
        first = done[1]
        done[1] = min(first + count, 8)
        if done[1] == first:
            return
        phase("choose")

        @pl.loop(first, done[1])
        def _(step):
            n = step // 2
            for u in range(8):
                at = lax.rem(step, 2) * 8 + u
                taken = pl.ds(pl.multiple_of(at * 256, 256), 256)
                pair = [gains.at[2 * n + i].reshape(ROWS * TERMS * 2, 128)[taken, :] for i in range(2)]
                value = dot(select[...], jnp.concatenate(pair, axis=1))
                for i in range(2):
                    half = value[:, i * 128 : (i + 1) * 128].astype(BF16)
                    chosen[2 * n + i, pl.ds(pl.multiple_of(at * 128, 128), 128), :] = half

    done = [0, 0]
    select[...] = (
        iota((128, 256), 1) == 2 * iota((128, 256), 0) + lax.rem(mz, 2)
    ).astype(F32).astype(BF16)
    bins_copy.wait()
    fracs_copy.wait()
    weigh_some(ROWS)
    for i, side in enumerate(SIDES):
        phase("near")
        wait_bytes(got_s, 8 if side else 7, rs_sem.at[side])
        for way in range(2):
            ring_copy(side, way).start()
        if i == 0:
            pltpu.make_async_copy(gains, gains, gain_sem).wait()
        choose_some(1)
    phase("meta")
    wait_bytes(got_m, NX - 1, rm_sem)
    row_at[mz] = jnp.sum(got_m[...].reshape(NX, 128), axis=0, keepdims=True)

    def row_copy(i):
        peer = (up, down, across)[i]
        return pltpu.make_async_remote_copy(
            src_ref=row_at.at[mz], dst_ref=row_at.at[mz], send_sem=ms_sem,
            recv_sem=mr_sem.at[i], device_id={"gx": mx, "gy": peer}, device_id_type=MESH,
        )

    for i in range(3):
        row_copy(i).start()

    half = iota((1, 2 * ND), 1) & 1
    twice = (iota((128, 2 * 128), 0) == iota((128, 2 * 128), 1) >> 1).astype(F32).astype(BF16)

    row_ids = iota((ROWS, 2 * 128), 0).astype(F32).astype(BF16)

    def plane_hits(z):
        row_of = dot(jnp.broadcast_to(row_at[z], (8, 128)).astype(BF16), twice)[0:1] - 1.0
        hits = [jnp.where(half == h, row_of, -1.0).astype(BF16) for h in range(2)]
        return [jnp.where(row_ids == hit, jnp.ones((), BF16), jnp.zeros((), BF16)) for hit in hits]

    def plane_sums(z, hits):
        data = got_s[pl.ds(z * NX, NX)].reshape(NX * 8, 512)
        return [dot(hit, data) for hit in hits]

    def add_plane(z, first):
        phase("plane")
        for h, part in enumerate(plane_sums(z, plane_hits(z))):
            lanes = slice(h * 512, (h + 1) * 512)
            sums[:, lanes] = part if first else sums[:, lanes] + part

    for i, side in enumerate(SIDES):
        if i == 1:
            add_plane(mz, True)
        choose_some(1)
        phase("relay")
        for way in range(2):
            ring_copy(side, way).wait_recv()
            relay_copy(side, way).start()
    for i in range(2):
        phase("rows")
        row_copy(i).wait_recv()
        add_plane((down, up)[i], False)
    choose_some(8)
    phase("arrive")
    row_copy(2).wait_recv()
    last_hits = plane_hits(across)
    wait_bytes(got_s, 32, zb_sem)

    phase("sums")
    for h, part in enumerate(plane_sums(across, last_hits)):
        part = part + sums[:, h * 512 : (h + 1) * 512]
        for k in range(4):
            rows[pl.ds(h * 4 + k, ROWS, stride=TERMS), :] = part[:, k * 128 : (k + 1) * 128]

    phase("binning")
    lane_row = (iota((PANELS, 128), 1) >> 3).astype(F32).astype(BF16)

    for batch in range(ROWS // 16):
        part = rows[batch * 128 : (batch + 1) * 128, :].astype(BF16).astype(F32)
        high = bins[pl.ds(batch * 16 * NZ + mz, 16, stride=NZ), :] >> 7
        high = [jnp.broadcast_to(high[g : g + 1, :], (TERMS, PANELS)) for g in range(16)]
        zero = jnp.where(jnp.concatenate(high, axis=0) == 0, part, 0.0)
        flats = [flat.T.astype(BF16) for flat in (zero, part - zero)]
        zeros = jnp.zeros((), BF16)
        wide = [
            jnp.concatenate([jnp.where(lane_row == g, flat, zeros) for flat in flats], axis=1)
            for g in range(16)
        ]
        tall = jnp.concatenate([weights[batch * 16 + g] for g in range(16)], axis=1)
        value = dot(tall, jnp.concatenate(wide, axis=0))
        low, high = value[0:HALF, 0:128], value[0:HALF, 128:256]
        carried = high[0:8] + value[HALF : HALF + 8, 0:128]
        arrived[batch, 0:HALF, :] = low.astype(BF16)
        arrived[batch, HALF:NBIN, :] = jnp.concatenate([carried, high[8:]], axis=0).astype(BF16)

    phase("signals")
    core = lax.rem(mx, 2)
    chip_x = (mx // 2) & 3
    sibling = mx + 1 - 2 * core
    near_half = chip_x >> 1

    def tiles_of(c):
        sides = (2, 1 + 2 * c, 3 - 2 * c, 0)
        halves = (1 - c, 1, 0, 1 - c)
        return [((my + side) & 3, (near_half + half) & 1) for side, half in zip(sides, halves)]

    theirs, mine = tiles_of(1 - core), tiles_of(core)

    def times_of(tiles):
        tall = jnp.concatenate([arrived[group] for group in range(16)], axis=1)
        value = dot(tall, jnp.concatenate([chosen[2 * y + half] for y, half in tiles], axis=1))
        return [value[:, i * 256 : (i + 1) * 256].T.reshape(32, 8, NBIN) for i in range(2)]

    def pair_copy(i):
        return pltpu.make_async_remote_copy(
            src_ref=send_q.at[i], dst_ref=got_q.at[i], send_sem=qs_sem, recv_sem=qr_sem.at[i],
            device_id={"gx": sibling, "gy": mz}, device_id_type=MESH,
        )

    def part_copy(tile, dx, dz, dc):
        y, half = mine[tile]
        x, c, z = ((chip_x + dx) & 1) + 2 * half, (core + dc) & 1, (mz + dz) & 3
        return pltpu.make_async_remote_copy(
            src_ref=send_p.at[tile, ((x & 1) * 2 + c) * NZ + z], dst_ref=got_p.at[mz * 16 + mx // 2],
            send_sem=sp_sem, recv_sem=rp_sem,
            device_id={"gx": y * 8 + x * 2 + c, "gy": z}, device_id_type=MESH,
        )

    for i, value in enumerate(times_of(theirs)):
        send_q[i] = value.astype(BF16)
        pair_copy(i).start()
    for i, value in enumerate(times_of(mine)):
        pair_copy(i).wait_recv()
        value = (value + got_q[i].astype(F32)).astype(BF16)
        for tile in (2 * i, 2 * i + 1):
            send_p[tile] = value[(tile & 1) * 16 : (tile & 1) * 16 + 16]
            for dz in (2, 1, 3, 0):
                for dx in (1, 0):
                    for dc in (1, 0):
                        if tile < 3 or dx or dz or dc:
                            part_copy(tile, dx, dz, dc).start()

    phase("collect")
    keeps = core == 1

    @pl.when(keeps)
    def _():
        got_p[mz * 16 + mx // 2] = send_p[3, ((chip_x & 1) * 2 + core) * NZ + mz]
        wait_bytes(got_p, 63, rp_sem)
        wait_bytes(got_p, 63, sp_sem)

    @pl.when(jnp.logical_not(keeps))
    def _():
        part_copy(3, 0, 0, 0).start()
        wait_bytes(got_p, 64, rp_sem)
        wait_bytes(got_p, 64, sp_sem)

    phase("total")
    for o in range(NZ):
        total = jnp.zeros((8, NBIN), F32)
        for i in range(16):
            total = total + got_p[o * 16 + i].astype(F32)
        out_ref[o] = total
    phase("drain")
    wait_bytes(got_s, NX - 1 + 64 + 32, ss_sem)
    wait_bytes(got_m, NX - 1, sm_sem)
    wait_bytes(row_at, 3, ms_sem)
    wait_bytes(send_q, 2, qs_sem)
    phase()


def on_device(sources, owners, strip_rows, panel_counts, arrival_bins, arrival_fracs, gain_table):
    any_space = pl.BlockSpec(memory_space=pl.ANY)
    vmem = pl.BlockSpec(memory_space=pltpu.VMEM)
    gains = gain_table.reshape(ROWS * TERMS, NZ, 8, 128).transpose(0, 2, 1, 3)
    gains = gains.reshape(ROWS * TERMS, 8, 2, 2, 128)
    dma = pltpu.SemaphoreType.DMA
    out = pl.pallas_call(
        kernel,
        out_shape=pltpu.VMEM((NZ, 8, NBIN), F32),
        in_specs=[any_space] * 7,
        out_specs=vmem,
        scratch_shapes=[
            pltpu.VMEM((NX, 8, 512), BF16),
            pltpu.VMEM((NX, 1, 128), F32),
            pltpu.VMEM((ND, 8, 512), BF16),
            pltpu.VMEM((NX, 1, 128), F32),
            pltpu.VMEM((ROWS * NZ, PANELS), I32),
            pltpu.VMEM((ROWS * NZ, PANELS), F32),
            pltpu.VMEM((8, ROWS * TERMS, 2, 128), BF16),
            pltpu.VMEM((ROWS, TALL, PANELS), BF16),
            pltpu.VMEM((ROWS * TERMS, PANELS), F32),
            pltpu.VMEM((16, NBIN, 128), BF16),
            pltpu.VMEM((8, ROWS * TERMS, 128), BF16),
            pltpu.VMEM((128, 256), BF16),
            pltpu.VMEM((ROWS, TERMS * PANELS), F32),
            pltpu.VMEM((NZ, 1, 128), F32),
            pltpu.VMEM((2, 32, 8, NBIN), BF16),
            pltpu.VMEM((2, 32, 8, NBIN), BF16),
            pltpu.VMEM((4, 16, 8, NBIN), BF16),
            pltpu.VMEM((64, 8, NBIN), BF16),
            dma((6,)), dma, dma, dma, dma, dma((4,)), dma, dma,
            dma((2, 4)), dma, dma, dma((3,)), dma, dma((2,)),
            pltpu.VMEM((STRIPS * TERMS, PANELS), BF16),
            pltpu.VMEM((1, STRIPS), I32), pltpu.VMEM((1, STRIPS), I32), pltpu.VMEM((1, STRIPS), I32),
        ],
        compiler_params=pltpu.CompilerParams(
            collective_id=0, has_side_effects=True, vmem_limit_bytes=60 * 1024 * 1024
        ),
    )(
        sources.reshape(STRIPS * TERMS, PANELS),
        owners.reshape(1, STRIPS),
        strip_rows.reshape(1, STRIPS),
        panel_counts.reshape(1, STRIPS),
        arrival_bins.reshape(ROWS * NZ, PANELS),
        arrival_fracs.reshape(ROWS * NZ, PANELS),
        gains,
    )
    return out.transpose(1, 0, 2)


def solution(mesh):
    placed = (
        P(("gx", "gy"), None, None),
        P(("gx", "gy"), None),
        P(("gx", "gy")),
        P(("gx", "gy")),
        P("gx", None, None),
        P("gx", None, None),
        P("gx", None, None, None),
    )
    return jax.shard_map(
        on_device,
        mesh=mesh,
        in_specs=placed,
        out_specs=P(("gx", "gy"), None, None),
        check_vma=False,
    )
```
